128 devices in a mesh: blk: 64 (over z, y, x_hi, core), head: 2 (over x_lo).
Axes of the slice: x: 4 (x_hi: 2, x_lo: 2; x = x_hi * 2 + x_lo), y: 4, z: 4, core: 2. Of those that a mesh axis runs over, the one named last changes fastest.
Arguments:
- queries: bfloat16 [16384, 1024], P('blk', 'head'), may hold values from -216 to 216
- keys: bfloat16 [16384, 1024], P('blk', 'head'), may hold values from -6 to 6
- values: bfloat16 [16384, 1024], P('blk', 'head'), may hold values from -6 to 6
- group_table: int32 [64, 2], P('blk'), may hold values from 0 to 127, as said below
- doc_ids: int32 [16384], replicated, may hold values from 0 to 15, never falling along the last dimension, each value on 1 to 8192 neighbouring positions
Outputs:
- attended: bfloat16 [16384, 1024], P('blk', 'head')
The draws below stay inside these ranges and needn't reach their ends.
Inputs may be any that keep to these rules, and one draw needn't show every extreme that they name: group_table[d, 1] = 127 - group_table[d, 0]; the first column holds each of 0 to 63 once. `doc_ids`: document numbers never fall along positions; a document holds at most 8192 positions.
All inputs are finite; a program needn't handle non-finite values.
Results may differ from the reference program's by a relative error of at most 0.0049.
Values may be sent and summed in bfloat16 or wider, within the bound.
A program may use at most 192 MiB of HBM per device.

```python
import math
import jax
import jax.numpy as jnp
import numpy as np
from jax import lax

HEAD_DIM = 128
HEADS = 8
TOK_DEV = 256
DOCS = 16
GROUP = 128
SEQ = 16384
MAXDOC = 8192
N_BLK = 64


def draw_queries(key, part):
    drawn = jnp.clip(jax.random.normal(jax.random.fold_in(key, 11), (SEQ, HEADS, HEAD_DIM), jnp.float32), -6.0, 6.0)
    return drawn.reshape(SEQ, HEADS * HEAD_DIM).astype(jnp.bfloat16)


def draw_keys(key, part):
    drawn = jnp.clip(jax.random.normal(jax.random.fold_in(key, 13), (SEQ, HEADS, HEAD_DIM), jnp.float32), -6.0, 6.0)
    return drawn.reshape(SEQ, HEADS * HEAD_DIM).astype(jnp.bfloat16)


def draw_group_table(key, part):
    order = jax.random.permutation(jax.random.fold_in(key, 17), N_BLK).astype(jnp.int32)
    return jnp.stack([order, 2 * N_BLK - 1 - order], axis=1).astype(jnp.int32)


def steps_of(key, extent, pieces, low, high):
    def one(dim, shards_of):
        heights = jax.random.uniform(jax.random.fold_in(jax.random.fold_in(key, 6), dim), (shards_of,), jnp.float32, low / len(pieces), high / len(pieces))
        return jnp.repeat(jnp.exp(heights), extent[dim] // shards_of).reshape((-1,) + (1,) * (len(extent) - dim - 1))

    loudness = one(*pieces[0])
    for cut in pieces[1:]:
        loudness = loudness * one(*cut)
    return loudness


def length_profile(amount, total, most, slope):
    loads = [(1 << 20) // math.isqrt(grade ** slope) + 1 for grade in range(2, amount + 1)]
    surplus, holding = total - most - (amount - 1), [1] * (amount - 1)
    while surplus > 0:
        candidates = [i for i in range(amount - 1) if holding[i] < most]
        whole, remaining = sum([loads[i] for i in candidates]), surplus
        for i in candidates:
            extra = min(most - holding[i], max(1, remaining * loads[i] // whole), surplus)
            holding[i] = holding[i] + extra
            surplus = surplus - extra
    return np.array([most] + holding)


def uneven(stream_key, count, total, most, slope):
    if count == 2:
        one = jax.random.randint(stream_key, (), max(1, total - most), min(most, total - 1) + 1)
        return jnp.stack([one, total - one])
    tallies = jnp.asarray(length_profile(count, total, most, slope), jnp.int32)
    twos = (count - 1) // 2
    donor, taker = tallies[1:1 + 2 * twos:2], tallies[2:2 + 2 * twos:2]
    margin = jnp.minimum(donor - 1, most - taker)
    passed = jax.random.randint(jax.random.fold_in(stream_key, 1), (twos,), 0, 1 << 20) % (margin + 1)
    tallies = tallies.at[1:1 + 2 * twos:2].set(donor - passed).at[2:2 + 2 * twos:2].set(taker + passed)
    return tallies[jax.random.permutation(jax.random.fold_in(stream_key, 2), count)]


def noise(rng, extent, deviation, reach, pieces=(), kind=jnp.bfloat16):
    values = jax.random.normal(rng, extent, jnp.float32) * deviation
    if len(pieces) > 0:
        values = steps_of(rng, extent, pieces, -0.22, 0.18) * values
    return jnp.clip(values, min=-reach, max=reach).astype(kind)


def setup_inputs(seed: int = 0) -> dict:
    streams_of = jax.random.split(jax.random.key(seed), 6)
    return {
        "queries": draw_queries(jax.random.fold_in(streams_of[5], 71), 0),
        "keys": draw_keys(jax.random.fold_in(streams_of[5], 71), 0),
        "values": noise(streams_of[2], (SEQ, HEADS * HEAD_DIM), 1.0, 6.0, ((0, 64), (1, 2))),
        "group_table": draw_group_table(jax.random.fold_in(streams_of[5], 71), 0),
        "doc_ids": jnp.searchsorted(jnp.cumsum(uneven(streams_of[4], DOCS, SEQ, MAXDOC, 2)), jnp.arange(SEQ), side="right").astype(jnp.int32),
    }


def reference(queries, keys, values, group_table, doc_ids):
    row_ids = jnp.arange(SEQ, dtype=jnp.int32)
    device = row_ids // TOK_DEV
    slot_ids = row_ids % TOK_DEV // GROUP
    position = (group_table[device, slot_ids] * GROUP + row_ids % GROUP).astype(jnp.int32)
    document = doc_ids[position]
    score_scale = 1.0 / math.sqrt(HEAD_DIM)
    query_block = math.gcd(SEQ, 1024)
    block_count = SEQ // query_block

    def one_head(head_index):
        start = (head_index * HEAD_DIM).astype(jnp.int32)
        head_queries = lax.dynamic_slice_in_dim(queries, start, HEAD_DIM, 1)
        head_keys = lax.dynamic_slice_in_dim(keys, start, HEAD_DIM, 1)
        head_values = lax.dynamic_slice_in_dim(values, start, HEAD_DIM, 1)

        def attend_block(args):
            query_rows, block_pos, block_doc = args
            scores = jnp.dot(query_rows, head_keys.T, preferred_element_type=jnp.float32) * score_scale
            visible = (block_doc[:, None] == document[None, :]) & (position[None, :] <= block_pos[:, None])
            rowmax = lax.optimization_barrier(jnp.max(jnp.where(visible, scores, -jnp.inf), axis=1))
            weights = jnp.where(visible, jnp.exp(scores - rowmax[:, None]), 0.0)
            denominator = lax.optimization_barrier(jnp.sum(weights, axis=1))
            output = jnp.dot(weights.astype(jnp.bfloat16), head_values, preferred_element_type=jnp.float32)
            return output / denominator[:, None]
        blocks = (head_queries.reshape(block_count, query_block, HEAD_DIM), position.reshape(block_count, query_block), document.reshape(block_count, query_block))
        return lax.map(attend_block, blocks).reshape(SEQ, HEAD_DIM)
    outputs = lax.map(one_head, jnp.arange(HEADS, dtype=jnp.int32))
    return jnp.transpose(outputs, (1, 0, 2)).reshape(SEQ, HEADS * HEAD_DIM).astype(jnp.bfloat16)
```

```python
import math

import jax
import jax.numpy as jnp
from jax import lax
from jax.experimental import pallas as pl
from jax.experimental.pallas import tpu as pltpu
from jax.sharding import Mesh
from jax.sharding import PartitionSpec as P

HEAD_DIM = 128
GROUP = 128
GROUPS = 128
AXES = ("z", "y", "xh", "core", "head")
BLK = AXES[:4]
MESH = pl.DeviceIdType.MESH
PART = 2 * GROUP + 16
NEG = -1e30
MASKED = -3e38
FAR = 1 << 20
TILE = 4
COEF = math.log2(math.e) / math.sqrt(HEAD_DIM)


def place():
    return tuple(lax.axis_index(a) for a in AXES)


def remote(src, dst, send, recv, to):
    return pltpu.make_async_remote_copy(
        src_ref=src, dst_ref=dst, send_sem=send, recv_sem=recv, device_id=to, device_id_type=MESH
    )


def spread_kernel(q_ref, k_ref, v_ref, table_ref, doc_ref, kv_out, q_out, start_out, src, loc, snd, own, yp, ym, rp, rm, dd, qr):
    z, y, xh, c, hd = place()
    up, down = lax.rem(y + 1, 4), lax.rem(y + 3, 4)
    zs = [z, lax.rem(z + 1, 4), lax.rem(z + 2, 4), lax.rem(z + 3, 4)]
    to_up, to_down, to_core = (z, up, xh, c, hd), (z, down, xh, c, hd), (z, y, xh, 1 - c, hd)
    partners = [(zs[dz], y, xh, c, hd) for dz in (1, 2, 3)]
    partners += [(zs[dz], y, 1 - xh, c, hd) for dz in range(4)] + [to_up, to_down, to_core]
    barrier = pltpu.get_barrier_semaphore()
    for to in partners:
        pl.semaphore_signal(barrier, inc=1, device_id=to, device_id_type=MESH)

    first = table_ref[0, 0].astype(jnp.float32)
    for h in range(4):
        cols = slice(h * HEAD_DIM, (h + 1) * HEAD_DIM)
        for s in range(2):
            rows = slice(s * GROUP, (s + 1) * GROUP)
            src[h, 0, rows, :] = k_ref[rows, cols]
            src[h, 1, rows, :] = v_ref[rows, cols].T
            src[h, 2, rows, :] = q_ref[rows, cols].T
        for p in range(3):
            src[h, p, 2 * GROUP :, :] = jnp.full((16, HEAD_DIM), first, jnp.float32).astype(jnp.bfloat16)
    docs = doc_ref[...]
    for d in range(16):
        counted = jnp.sum(jnp.where(docs < d, 1, 0), axis=0, keepdims=True)
        start_out[d : d + 1, :] = jnp.broadcast_to(jnp.sum(counted, axis=1, keepdims=True), (1, 128))
    pl.semaphore_wait(barrier, len(partners))

    sent = []

    def start(src_ref, dst_ref, recv, to):
        copy = remote(src_ref, dst_ref, snd.at[len(sent)], recv, to)
        copy.start()
        sent.append(copy)

    def landed(dst_ref, recv):
        remote(dst_ref, dst_ref, snd.at[0], recv, to_core).wait_recv()

    def chunk(zz, yy, cc):
        return kv_out.at[(zz * 4 + yy) * 2 + cc]

    order = (0, 1, 3, 2)
    for dz in order[1:]:
        start(src.at[zs[dz], pl.ds(0, 2)], chunk(z, y, c), own.at[dz], (zs[dz], y, xh, c, hd))
    keep = pltpu.make_async_copy(src.at[z, pl.ds(0, 2)], chunk(z, y, c), loc.at[0])
    keep.start()
    came = [zs[(4 - dz) % 4] for dz in order]

    def first_hop(s):
        mine = chunk(came[s], y, c)
        here = src.at[z, pl.ds(0, 2)]
        if s > 0:
            landed(mine, own.at[order[s]])
            here = mine
        start(here, mine, yp.at[s], to_up)
        start(here, mine, ym.at[s], to_down)
        start(here, mine, dd.at[s, 0], to_core)

    def second_hop(s):
        below, above = chunk(came[s], down, c), chunk(came[s], up, c)
        landed(below, yp.at[s])
        start(below.at[0], below.at[0], rp.at[s], to_up)
        start(below, below, dd.at[s, 1], to_core)
        landed(above, ym.at[s])
        start(above.at[1], above.at[1], rm.at[s], to_down)
        start(above, above, dd.at[s, 2], to_core)

    def last_hop(s):
        across = chunk(came[s], lax.rem(y + 2, 4), c)
        landed(across.at[0], rp.at[s])
        start(across.at[0], across.at[0], dd.at[s, 3], to_core)
        landed(across.at[1], rm.at[s])
        start(across.at[1], across.at[1], dd.at[s, 4], to_core)

    first_hop(0)
    q_mine = q_out.at[z * 2 + xh]
    keep_q = pltpu.make_async_copy(src.at[z, 2], q_mine, loc.at[1])
    keep_q.start()
    for dz in (1, 3, 2, 0):
        for dx in (1, 0):
            if dz or dx:
                to = (zs[dz], y, 1 - xh if dx else xh, c, hd)
                start(src.at[zs[dz], 2], q_mine, qr.at[dz * 2 + dx], to)
    first_hop(1)
    second_hop(0)
    first_hop(2)
    second_hop(1)
    last_hop(0)
    first_hop(3)
    second_hop(2)
    last_hop(1)
    second_hop(3)
    last_hop(2)
    last_hop(3)

    for dz in range(4):
        for dx in range(2):
            if dz or dx:
                landed(q_out.at[zs[(4 - dz) % 4] * 2 + (1 - xh if dx else xh)], qr.at[dz * 2 + dx])
    for s in range(4):
        other = [chunk(came[s], yy, 1 - c) for yy in (y, down, up, lax.rem(y + 2, 4))]
        for i in range(3):
            landed(other[i], dd.at[s, i])
        landed(other[3].at[0], dd.at[s, 3])
        landed(other[3].at[1], dd.at[s, 4])
    keep.wait()
    keep_q.wait()
    for copy in sent:
        copy.wait_send()


def attend_kernel(kv_hbm, q_hbm, start_hbm, o_ref, l_ref, kv, q, hdr_k, hdr_q, tabv, tabs, starts, inv, lst, pre, sems):
    small = [
        pltpu.make_async_copy(kv_hbm.at[:, 0, pl.ds(2 * GROUP, 16), :], hdr_k, sems.at[0]),
        pltpu.make_async_copy(q_hbm.at[:, pl.ds(2 * GROUP, 16), :], hdr_q, sems.at[1]),
        pltpu.make_async_copy(start_hbm, starts, sems.at[2]),
    ]
    large = [pltpu.make_async_copy(q_hbm, q, sems.at[3])]
    for i in range(4):
        large.append(pltpu.make_async_copy(kv_hbm.at[pl.ds(8 * i, 8)], kv.at[pl.ds(8 * i, 8)], sems.at[4 + i]))
    for copy in small + large:
        copy.start()
    for copy in small:
        copy.wait()
    tabv[0:32, :] = hdr_k[:, 0, :].astype(jnp.float32).astype(jnp.int32)
    tabv[32:40, :] = hdr_q[:, 0, :].astype(jnp.float32).astype(jnp.int32)
    table_copy = pltpu.make_async_copy(tabv, tabs, sems.at[8])
    table_copy.start()

    @pl.loop(0, GROUPS)
    def _(p):
        inv[p] = -1

    table_copy.wait()

    @pl.loop(0, 32)
    def _(i):
        g0 = tabs[i, 0]
        inv[g0] = 2 * i
        inv[GROUPS - 1 - g0] = 2 * i + 1

    def count(p, n):
        pre[p] = n
        lst[n] = inv[p] * GROUPS + p
        return n + jnp.where(inv[p] >= 0, 1, 0)

    pre[GROUPS] = lax.fori_loop(0, GROUPS, count, jnp.int32(0))
    for copy in large:
        copy.wait()

    lane = lax.broadcasted_iota(jnp.int32, (1, GROUP), 1)
    row = lax.broadcasted_iota(jnp.int32, (GROUP, GROUP), 0)

    @pl.loop(0, 16)
    def _(u):
        ch, s = lax.div(u, 2), lax.rem(u, 2)
        g0 = tabs[32 + ch, 0]
        g = jnp.where(s == 0, g0, GROUPS - 1 - g0)
        at = pl.ds(pl.multiple_of(s * GROUP, GROUP), GROUP)
        q_t = q[ch, at, :]
        qpos = g * GROUP + lane
        low, low_first = jnp.zeros_like(lane), jnp.int32(0)
        for d in range(1, 16):
            begin = starts[d, 0]
            low = jnp.where(begin <= qpos, begin, low)
            low_first = jnp.where(begin <= g * GROUP, begin, low_first)
        begin_at, end_at = pre[lax.div(low_first, GROUP)], pre[g + 1]

        def step(t, state):
            top, weight, acc = state
            scores, held = [], []
            for i in range(TILE):
                e = begin_at + t * TILE + i
                entry = lst[jnp.minimum(e, end_at - 1)]
                slot, key_group = lax.div(entry, GROUPS), lax.rem(entry, GROUPS)
                base = jnp.where(e < end_at, key_group * GROUP, FAR)
                where = pl.ds(pl.multiple_of(lax.rem(slot, 2) * GROUP, GROUP), GROUP)
                one = jnp.dot(kv[lax.div(slot, 2), 0, where, :], q_t, preferred_element_type=jnp.float32)
                seen = (row >= low - base) & (row <= qpos - base)
                scores.append(jnp.where(seen, one, MASKED))
                held.append(kv[lax.div(slot, 2), 1, where, :])
            new_top = top
            for one in scores:
                new_top = jnp.maximum(new_top, jnp.max(one, axis=0, keepdims=True))
            factor = jnp.exp2((top - new_top) * COEF)
            weight, acc = weight * factor, acc * factor
            for one, v_t in zip(scores, held):
                part = jnp.exp2((one - new_top) * COEF)
                weight = weight + jnp.sum(part, axis=0, keepdims=True)
                acc = acc + jnp.dot(v_t, part.astype(jnp.bfloat16), preferred_element_type=jnp.float32)
            return new_top, weight, acc

        top, weight, acc = lax.fori_loop(
            0,
            lax.div(end_at - begin_at + TILE - 1, TILE),
            step,
            (
                jnp.full((1, GROUP), NEG, jnp.float32),
                jnp.zeros((1, GROUP), jnp.float32),
                jnp.zeros((HEAD_DIM, GROUP), jnp.float32),
            ),
        )
        some = weight > 0.0
        safe = jnp.where(some, weight, 1.0)
        o_ref[ch, at, :] = (acc / safe).astype(jnp.bfloat16)
        l_ref[ch, pl.ds(s, 1), :] = jnp.where(some, top * COEF + jnp.log2(safe), NEG)


def merge_kernel(o_hbm, l_hbm, out_ref, o_in, l_in, loc, snd, orecv, lrecv):
    z, y, xh, c, hd = place()
    zs = [z, lax.rem(z + 1, 4), lax.rem(z + 2, 4), lax.rem(z + 3, 4)]
    peers = [(dz, dx) for dz in (2, 1, 3, 0) for dx in (1, 0) if dz or dx]
    barrier = pltpu.get_barrier_semaphore()
    for dz, dx in peers:
        to = (zs[dz], y, 1 - xh if dx else xh, c, hd)
        pl.semaphore_signal(barrier, inc=1, device_id=to, device_id_type=MESH)
    mine = z * 2 + xh
    keep = [
        pltpu.make_async_copy(o_hbm.at[mine], o_in.at[mine], loc.at[0]),
        pltpu.make_async_copy(l_hbm.at[mine], l_in.at[mine], loc.at[1]),
    ]
    for copy in keep:
        copy.start()
    pl.semaphore_wait(barrier, len(peers))
    sent = []
    for n, (dz, dx) in enumerate(peers):
        side = 1 - xh if dx else xh
        to, theirs = (zs[dz], y, side, c, hd), zs[dz] * 2 + side
        for src, dst, recv in ((o_hbm, o_in, orecv), (l_hbm, l_in, lrecv)):
            copy = remote(src.at[theirs], dst.at[mine], snd.at[len(sent)], recv.at[dz * 2 + dx], to)
            copy.start()
            sent.append(copy)
    for copy in keep:
        copy.wait()
    for dz, dx in peers:
        side = 1 - xh if dx else xh
        theirs = zs[(4 - dz) % 4] * 2 + side
        to = (zs[1], y, xh, c, hd)
        remote(o_hbm.at[0], o_in.at[theirs], snd.at[0], orecv.at[dz * 2 + dx], to).wait_recv()
        remote(l_hbm.at[0], l_in.at[theirs], snd.at[0], lrecv.at[dz * 2 + dx], to).wait_recv()
    for h in range(4):
        for s in range(2):
            rows = slice(s * GROUP, (s + 1) * GROUP)
            a, b = l_in[2 * h, s : s + 1, :], l_in[2 * h + 1, s : s + 1, :]
            most = jnp.maximum(a, b)
            wa, wb = jnp.exp2(a - most), jnp.exp2(b - most)
            total = wa + wb
            merged = o_in[2 * h, rows, :].astype(jnp.float32) * (wa / total)
            merged = merged + o_in[2 * h + 1, rows, :].astype(jnp.float32) * (wb / total)
            out_ref[rows, h * HEAD_DIM : (h + 1) * HEAD_DIM] = merged.T.astype(jnp.bfloat16)
    for copy in sent:
        copy.wait_send()


def shards(queries, keys, values, group_table, doc_ids):
    vmem = pl.BlockSpec(memory_space=pltpu.VMEM)
    hbm = pl.BlockSpec(memory_space=pl.ANY)
    smem = pl.BlockSpec(memory_space=pltpu.SMEM)
    dma = pltpu.SemaphoreType.DMA
    kv, q, begins = pl.pallas_call(
        spread_kernel,
        out_shape=(
            jax.ShapeDtypeStruct((32, 2, PART, HEAD_DIM), jnp.bfloat16),
            jax.ShapeDtypeStruct((8, PART, HEAD_DIM), jnp.bfloat16),
            jax.ShapeDtypeStruct((16, 128), jnp.int32),
        ),
        in_specs=[vmem, vmem, vmem, smem, vmem],
        out_specs=(hbm, hbm, vmem),
        scratch_shapes=[
            pltpu.VMEM((4, 3, PART, HEAD_DIM), jnp.bfloat16),
            dma((2,)), dma((46,)), dma((4,)), dma((4,)), dma((4,)), dma((4,)), dma((4,)), dma((4, 5)), dma((8,)),
        ],
        compiler_params=pltpu.CompilerParams(collective_id=0, has_side_effects=True),
    )(queries, keys, values, group_table, doc_ids.reshape(128, 128))
    o, l = pl.pallas_call(
        attend_kernel,
        out_shape=(
            jax.ShapeDtypeStruct((8, 2 * GROUP, HEAD_DIM), jnp.bfloat16),
            jax.ShapeDtypeStruct((8, 8, GROUP), jnp.float32),
        ),
        in_specs=[hbm, hbm, hbm],
        out_specs=(vmem, vmem),
        scratch_shapes=[
            pltpu.VMEM((32, 2, PART, HEAD_DIM), jnp.bfloat16),
            pltpu.VMEM((8, PART, HEAD_DIM), jnp.bfloat16),
            pltpu.VMEM((32, 16, HEAD_DIM), jnp.bfloat16),
            pltpu.VMEM((8, 16, HEAD_DIM), jnp.bfloat16),
            pltpu.VMEM((40, 128), jnp.int32),
            pltpu.SMEM((40, 128), jnp.int32),
            pltpu.SMEM((16, 128), jnp.int32),
            pltpu.SMEM((GROUPS,), jnp.int32),
            pltpu.SMEM((GROUPS,), jnp.int32),
            pltpu.SMEM((GROUPS + 8,), jnp.int32),
            dma((9,)),
        ],
    )(kv, q, begins)
    return pl.pallas_call(
        merge_kernel,
        out_shape=jax.ShapeDtypeStruct(queries.shape, jnp.bfloat16),
        in_specs=[hbm, hbm],
        out_specs=vmem,
        scratch_shapes=[
            pltpu.VMEM((8, 2 * GROUP, HEAD_DIM), jnp.bfloat16),
            pltpu.VMEM((8, 8, GROUP), jnp.float32),
            dma((2,)), dma((14,)), dma((8,)), dma((8,)),
        ],
        compiler_params=pltpu.CompilerParams(collective_id=1, has_side_effects=True),
    )(o, l)


def solution(mesh):
    split = Mesh(mesh.devices.reshape(4, 4, 2, 2, mesh.shape["head"]), AXES)
    return jax.shard_map(
        shards,
        mesh=split,
        in_specs=(P(BLK, "head"), P(BLK, "head"), P(BLK, "head"), P(BLK, None), P()),
        out_specs=P(BLK, "head"),
        check_vma=False,
    )
```

```python
import math

import jax
import jax.numpy as jnp
from jax import lax
from jax.experimental import pallas as pl
from jax.experimental.pallas import tpu as pltpu
from jax.sharding import Mesh
from jax.sharding import PartitionSpec as P

HEAD_DIM = 128
GROUP = 128
GROUPS = 128
AXES = ("z", "y", "xh", "core", "head")
BLK = AXES[:4]
MESH = pl.DeviceIdType.MESH
PART = 2 * GROUP + 16
NEG = -1e30
MASKED = -3e38
FAR = 1 << 20
TILE = 4
COEF = math.log2(math.e) / math.sqrt(HEAD_DIM)


def place():
    return tuple(lax.axis_index(a) for a in AXES)


def remote(src, dst, send, recv, to):
    return pltpu.make_async_remote_copy(
        src_ref=src, dst_ref=dst, send_sem=send, recv_sem=recv, device_id=to, device_id_type=MESH
    )


def spread_kernel(q_ref, k_ref, v_ref, table_ref, doc_ref, kv_out, q_out, start_out, src, snd, own, yp, ym, rp, rm, dd, qr):
    z, y, xh, c, hd = place()
    up, down = lax.rem(y + 1, 4), lax.rem(y + 3, 4)
    zs = [z, lax.rem(z + 1, 4), lax.rem(z + 2, 4), lax.rem(z + 3, 4)]
    to_up, to_down, to_core = (z, up, xh, c, hd), (z, down, xh, c, hd), (z, y, xh, 1 - c, hd)
    partners = [(zs[dz], y, xh, c, hd) for dz in (1, 2, 3)]
    partners += [(zs[dz], y, 1 - xh, c, hd) for dz in range(4)] + [to_up, to_down, to_core]
    barrier = pltpu.get_barrier_semaphore()
    for to in partners:
        pl.semaphore_signal(barrier, inc=1, device_id=to, device_id_type=MESH)

    first = table_ref[0, 0].astype(jnp.float32)
    for h in range(4):
        cols = slice(h * HEAD_DIM, (h + 1) * HEAD_DIM)
        for s in range(2):
            rows = slice(s * GROUP, (s + 1) * GROUP)
            src[h, 0, rows, :] = k_ref[rows, cols]
            src[h, 1, rows, :] = v_ref[rows, cols].T
            src[h, 2, rows, :] = q_ref[rows, cols].T
        for p in range(3):
            src[h, p, 2 * GROUP :, :] = jnp.full((16, HEAD_DIM), first, jnp.float32).astype(jnp.bfloat16)
    docs = doc_ref[...]
    for d in range(16):
        counted = jnp.sum(jnp.where(docs < d, 1, 0), axis=0, keepdims=True)
        start_out[d : d + 1, :] = jnp.broadcast_to(jnp.sum(counted, axis=1, keepdims=True), (1, 128))
    pl.semaphore_wait(barrier, len(partners))

    sent = []

    def start(src_ref, dst_ref, recv, to):
        copy = remote(src_ref, dst_ref, snd.at[len(sent)], recv, to)
        copy.start()
        sent.append(copy)

    def landed(dst_ref, recv):
        remote(dst_ref, dst_ref, snd.at[0], recv, to_core).wait_recv()

    def chunk(zz, yy, cc):
        return kv_out.at[(zz * 4 + yy) * 2 + cc]

    order = (0, 1, 3, 2)
    for dz in order[1:]:
        start(src.at[zs[dz], pl.ds(0, 2)], chunk(z, y, c), own.at[dz], (zs[dz], y, xh, c, hd))
    kv_out[(z * 4 + y) * 2 + c] = src[z, 0:2]
    came = [zs[(4 - dz) % 4] for dz in order]

    def first_hop(s):
        mine = chunk(came[s], y, c)
        here = src.at[z, pl.ds(0, 2)]
        if s > 0:
            landed(mine, own.at[order[s]])
            here = mine
        start(here, mine, yp.at[s], to_up)
        start(here, mine, ym.at[s], to_down)
        start(here, mine, dd.at[s, 0], to_core)

    def second_hop(s):
        below, above = chunk(came[s], down, c), chunk(came[s], up, c)
        landed(below, yp.at[s])
        start(below.at[0], below.at[0], rp.at[s], to_up)
        start(below, below, dd.at[s, 1], to_core)
        landed(above, ym.at[s])
        start(above.at[1], above.at[1], rm.at[s], to_down)
        start(above, above, dd.at[s, 2], to_core)

    def last_hop(s):
        across = chunk(came[s], lax.rem(y + 2, 4), c)
        landed(across.at[0], rp.at[s])
        start(across.at[0], across.at[0], dd.at[s, 3], to_core)
        landed(across.at[1], rm.at[s])
        start(across.at[1], across.at[1], dd.at[s, 4], to_core)

    first_hop(0)
    q_mine = q_out.at[z * 2 + xh]
    q_out[z * 2 + xh] = src[z, 2]
    for dz in (1, 3, 2, 0):
        for dx in (1, 0):
            if dz or dx:
                to = (zs[dz], y, 1 - xh if dx else xh, c, hd)
                start(src.at[zs[dz], 2], q_mine, qr.at[dz * 2 + dx], to)
    first_hop(1)
    second_hop(0)
    first_hop(2)
    second_hop(1)
    last_hop(0)
    first_hop(3)
    second_hop(2)
    last_hop(1)
    second_hop(3)
    last_hop(2)
    last_hop(3)

    for dz in range(4):
        for dx in range(2):
            if dz or dx:
                landed(q_out.at[zs[(4 - dz) % 4] * 2 + (1 - xh if dx else xh)], qr.at[dz * 2 + dx])
    for s in range(4):
        other = [chunk(came[s], yy, 1 - c) for yy in (y, down, up, lax.rem(y + 2, 4))]
        for i in range(3):
            landed(other[i], dd.at[s, i])
        landed(other[3].at[0], dd.at[s, 3])
        landed(other[3].at[1], dd.at[s, 4])
    for copy in sent:
        copy.wait_send()


def attend_kernel(kv, q, start_ref, o_ref, l_ref, plan, sm, low_s, bias_s, top_s, weight_s, acc_s, s_even, s_odd, sem):
    lane = lax.broadcasted_iota(jnp.int32, (1, 128), 1)
    lane32 = lax.broadcasted_iota(jnp.int32, (32, 128), 1)
    lane16 = lax.broadcasted_iota(jnp.int32, (16, 128), 1)
    code = lax.broadcasted_iota(jnp.int32, (32, 128), 0) * 2
    first = kv[:, 0, 2 * GROUP, :].astype(jnp.float32).astype(jnp.int32)
    second = GROUPS - 1 - first
    at = jnp.where(first == lane32, code + 1, 0) + jnp.where(second == lane32, code + 2, 0)
    inv = jnp.sum(at, axis=0, keepdims=True) - 1
    here = jnp.where(inv >= 0, 1, 0)
    rank0 = jnp.sum(jnp.where(lane32 < first, here, 0), axis=1, keepdims=True)
    rank1 = jnp.sum(jnp.where(lane32 < second, here, 0), axis=1, keepdims=True)
    listed = jnp.where(rank0 == lane32, code * GROUPS, 0) + jnp.where(rank1 == lane32, (code + 1) * GROUPS, 0)
    plan[0:1, :] = jnp.sum(listed, axis=0, keepdims=True)
    plan[1:2, :] = inv

    q_first = q[:, 2 * GROUP, :].astype(jnp.float32).astype(jnp.int32)
    group = jnp.concatenate([q_first, GROUPS - 1 - q_first], axis=0)
    q_pos = group * GROUP + lane16
    low, low_first = jnp.zeros_like(q_pos), jnp.zeros_like(q_pos)
    for d in range(1, 16):
        begin = start_ref[d : d + 1, :]
        low = jnp.where(begin <= q_pos, begin, low)
        low_first = jnp.where(begin <= group * GROUP, begin, low_first)
    low_s[...] = low
    bias_s[...] = jnp.where(low == low_first, 0.0, MASKED)
    low_group = lax.shift_right_logical(low_first, 7)
    plan[16:32, :] = group
    plan[32:48, :] = low_group
    begin_at = jnp.sum(jnp.where(lane16 <= low_group, here, 0), axis=1, keepdims=True)
    end_at = jnp.sum(jnp.where(lane16 < group, here, 0), axis=1, keepdims=True)
    tiles = lax.shift_right_logical(jnp.maximum(end_at - begin_at, 0) + (TILE - 1), 2)
    begin_at, end_at, tiles = (jnp.broadcast_to(x, (16, 128)) for x in (begin_at, end_at, tiles))
    done = jnp.zeros((1, 128), jnp.int32)
    item = [lane, lane + 128, lane + 256]
    item_u, item_at, item_end = [[jnp.zeros((1, 128), jnp.int32) for _ in item] for _ in range(3)]
    for u in range(16):
        after = done + tiles[u : u + 1, :]
        for i, n in enumerate(item):
            mine = (done <= n) & (n < after)
            item_u[i] = jnp.where(mine, u, item_u[i])
            item_at[i] = jnp.where(mine, begin_at[u : u + 1, :] + (n - done) * TILE, item_at[i])
            item_end[i] = jnp.where(mine, end_at[u : u + 1, :], item_end[i])
        done = after
    for i in range(3):
        plan[2 + i : 3 + i, :] = item_u[i]
        plan[5 + i : 6 + i, :] = item_at[i]
        plan[8 + i : 9 + i, :] = item_end[i]
    plan[11:12, :] = done
    copy = pltpu.make_async_copy(plan, sm, sem)
    copy.start()
    copy.wait()

    row = lax.broadcasted_iota(jnp.int32, (GROUP, GROUP), 0)

    def half(slot):
        return pl.ds(pl.multiple_of(lax.rem(slot, 2) * GROUP, GROUP), GROUP)

    def queries_of(u):
        return q[lax.rem(u, 8), pl.ds(pl.multiple_of(lax.div(u, 8) * GROUP, GROUP), GROUP), :]

    @pl.loop(0, 16)
    def _(u):
        g, low_g = sm[16 + u, 0], sm[32 + u, 0]
        q_t = queries_of(u)
        lower = low_s[pl.ds(u, 1), :]
        upper = g * GROUP + lane
        scores, held = [], []
        for key_group, wanted in ((g, True), (low_g, low_g < g)):
            found = sm[1, key_group]
            slot = jnp.maximum(found, 0)
            base = jnp.where((found >= 0) & wanted, key_group * GROUP, FAR)
            one = jnp.dot(kv[lax.div(slot, 2), 0, half(slot), :], q_t, preferred_element_type=jnp.float32)
            seen = (row >= lower - base) & (row <= upper - base)
            scores.append(jnp.where(seen, one, MASKED))
            held.append(kv[lax.div(slot, 2), 1, half(slot), :])
        top = jnp.full((1, GROUP), NEG, jnp.float32)
        for one in scores:
            top = jnp.maximum(top, jnp.max(one, axis=0, keepdims=True))
        parts = [jnp.exp2((one - top) * COEF) for one in scores]
        top_s[pl.ds(u, 1), :] = top
        weight_s[pl.ds(u, 1), :] = sum(jnp.sum(part, axis=0, keepdims=True) for part in parts)
        acc_s[u] = jnp.dot(
            jnp.concatenate(held, axis=1),
            jnp.concatenate([part.astype(jnp.bfloat16) for part in parts], axis=0),
            preferred_element_type=jnp.float32,
        )

    def read(i):
        r, k = lax.shift_right_logical(i, 7), lax.bitwise_and(i, 127)
        return sm[2 + r, k], sm[5 + r, k], sm[8 + r, k]

    def slot_of(e, end):
        return lax.shift_right_logical(sm[0, jnp.maximum(jnp.minimum(e, end - 1), 0)], 7)

    def score(i, dst):
        u, e, end = read(i)
        q_t = queries_of(u)
        for j in range(TILE):
            slot = slot_of(e + j, end)
            dst[j * GROUP : (j + 1) * GROUP, :] = jnp.dot(
                kv[lax.div(slot, 2), 0, half(slot), :], q_t, preferred_element_type=jnp.float32
            )

    def absorb(i, src):
        u, e, end = read(i)
        lanes = bias_s[pl.ds(u, 1), :]
        top = top_s[pl.ds(u, 1), :]
        new_top, biases, held, parts = top, [], [], []
        for j in range(TILE):
            biases.append(jnp.where(e + j < end, lanes, MASKED))
            best = jnp.max(src[j * GROUP : (j + 1) * GROUP, :], axis=0, keepdims=True)
            new_top = jnp.maximum(new_top, best + biases[j])
        factor = jnp.exp2((top - new_top) * COEF)
        weight = weight_s[pl.ds(u, 1), :] * factor
        for j in range(TILE):
            part = jnp.exp2((src[j * GROUP : (j + 1) * GROUP, :] - (new_top - biases[j])) * COEF)
            weight = weight + jnp.sum(part, axis=0, keepdims=True)
            parts.append(part.astype(jnp.bfloat16))
            slot = slot_of(e + j, end)
            held.append(kv[lax.div(slot, 2), 1, half(slot), :])
        top_s[pl.ds(u, 1), :] = new_top
        weight_s[pl.ds(u, 1), :] = weight
        acc_s[u] = acc_s[u] * factor + jnp.dot(
            jnp.concatenate(held, axis=1), jnp.concatenate(parts, axis=0), preferred_element_type=jnp.float32
        )

    total = sm[11, 0]
    score(jnp.int32(0), s_even)

    @pl.loop(0, lax.shift_right_logical(total + 1, 1))
    def _(k):
        i = 2 * k
        score(i + 1, s_odd)
        absorb(i, s_even)
        score(i + 2, s_even)
        absorb(i + 1, s_odd)

    @pl.loop(0, 16)
    def _(u):
        weight = weight_s[pl.ds(u, 1), :]
        some = weight > 0.0
        safe = jnp.where(some, weight, 1.0)
        ch, s = lax.rem(u, 8), lax.div(u, 8)
        o_ref[ch, pl.ds(pl.multiple_of(s * GROUP, GROUP), GROUP), :] = (acc_s[u] * (1.0 / safe)).astype(jnp.bfloat16)
        l_ref[ch, pl.ds(s, 1), :] = jnp.where(some, top_s[pl.ds(u, 1), :] * COEF + jnp.log2(safe), NEG)


def merge_kernel(o_ref, l_ref, out_ref, o_in, l_in, snd, orecv, lrecv):
    z, y, xh, c, hd = place()
    zs = [z, lax.rem(z + 1, 4), lax.rem(z + 2, 4), lax.rem(z + 3, 4)]
    peers = [(dz, dx) for dz in (2, 1, 3, 0) for dx in (1, 0) if dz or dx]
    barrier = pltpu.get_barrier_semaphore()
    for dz, dx in peers:
        to = (zs[dz], y, 1 - xh if dx else xh, c, hd)
        pl.semaphore_signal(barrier, inc=1, device_id=to, device_id_type=MESH)
    mine = z * 2 + xh
    o_in[mine] = o_ref[mine]
    l_in[mine] = l_ref[mine]
    pl.semaphore_wait(barrier, len(peers))
    sent = []
    for n, (dz, dx) in enumerate(peers):
        side = 1 - xh if dx else xh
        to, theirs = (zs[dz], y, side, c, hd), zs[dz] * 2 + side
        for src, dst, recv in ((o_ref, o_in, orecv), (l_ref, l_in, lrecv)):
            copy = remote(src.at[theirs], dst.at[mine], snd.at[len(sent)], recv.at[dz * 2 + dx], to)
            copy.start()
            sent.append(copy)
    for dz, dx in peers:
        side = 1 - xh if dx else xh
        theirs = zs[(4 - dz) % 4] * 2 + side
        to = (zs[1], y, xh, c, hd)
        remote(o_ref.at[0], o_in.at[theirs], snd.at[0], orecv.at[dz * 2 + dx], to).wait_recv()
        remote(l_ref.at[0], l_in.at[theirs], snd.at[0], lrecv.at[dz * 2 + dx], to).wait_recv()
    for h in range(4):
        for s in range(2):
            rows = slice(s * GROUP, (s + 1) * GROUP)
            a, b = l_in[2 * h, s : s + 1, :], l_in[2 * h + 1, s : s + 1, :]
            most = jnp.maximum(a, b)
            wa, wb = jnp.exp2(a - most), jnp.exp2(b - most)
            total = wa + wb
            merged = o_in[2 * h, rows, :].astype(jnp.float32) * (wa / total)
            merged = merged + o_in[2 * h + 1, rows, :].astype(jnp.float32) * (wb / total)
            out_ref[rows, h * HEAD_DIM : (h + 1) * HEAD_DIM] = merged.T.astype(jnp.bfloat16)
    for copy in sent:
        copy.wait_send()


def shards(queries, keys, values, group_table, doc_ids):
    vmem = pl.BlockSpec(memory_space=pltpu.VMEM)
    hbm = pl.BlockSpec(memory_space=pl.ANY)
    smem = pl.BlockSpec(memory_space=pltpu.SMEM)
    dma = pltpu.SemaphoreType.DMA
    kv, q, begins = pl.pallas_call(
        spread_kernel,
        out_shape=(
            pltpu.VMEM((32, 2, PART, HEAD_DIM), jnp.bfloat16),
            pltpu.VMEM((8, PART, HEAD_DIM), jnp.bfloat16),
            pltpu.VMEM((16, 128), jnp.int32),
        ),
        in_specs=[vmem, vmem, vmem, smem, vmem],
        out_specs=(vmem, vmem, vmem),
        scratch_shapes=[
            pltpu.VMEM((4, 3, PART, HEAD_DIM), jnp.bfloat16),
            dma((46,)), dma((4,)), dma((4,)), dma((4,)), dma((4,)), dma((4,)), dma((4, 5)), dma((8,)),
        ],
        compiler_params=pltpu.CompilerParams(collective_id=0, has_side_effects=True, vmem_limit_bytes=16 << 20),
    )(queries, keys, values, group_table, doc_ids.reshape(128, 128))
    o, l = pl.pallas_call(
        attend_kernel,
        out_shape=(
            pltpu.VMEM((8, 2 * GROUP, HEAD_DIM), jnp.bfloat16),
            pltpu.VMEM((8, 8, GROUP), jnp.float32),
        ),
        in_specs=[vmem, vmem, vmem],
        out_specs=(vmem, vmem),
        scratch_shapes=[
            pltpu.VMEM((48, 128), jnp.int32),
            pltpu.SMEM((48, 128), jnp.int32),
            pltpu.VMEM((16, 128), jnp.int32),
            pltpu.VMEM((16, 128), jnp.float32),
            pltpu.VMEM((16, 128), jnp.float32),
            pltpu.VMEM((16, 128), jnp.float32),
            pltpu.VMEM((16, HEAD_DIM, GROUP), jnp.float32),
            pltpu.VMEM((TILE * GROUP, GROUP), jnp.float32),
            pltpu.VMEM((TILE * GROUP, GROUP), jnp.float32),
            dma,
        ],
        compiler_params=pltpu.CompilerParams(vmem_limit_bytes=16 << 20),
    )(kv, q, begins)
    return pl.pallas_call(
        merge_kernel,
        out_shape=jax.ShapeDtypeStruct(queries.shape, jnp.bfloat16),
        in_specs=[vmem, vmem],
        out_specs=vmem,
        scratch_shapes=[
            pltpu.VMEM((8, 2 * GROUP, HEAD_DIM), jnp.bfloat16),
            pltpu.VMEM((8, 8, GROUP), jnp.float32),
            dma((14,)), dma((8,)), dma((8,)),
        ],
        compiler_params=pltpu.CompilerParams(collective_id=1, has_side_effects=True, vmem_limit_bytes=16 << 20),
    )(o, l)


def solution(mesh):
    split = Mesh(mesh.devices.reshape(4, 4, 2, 2, mesh.shape["head"]), AXES)
    return jax.shard_map(
        shards,
        mesh=split,
        in_specs=(P(BLK, "head"), P(BLK, "head"), P(BLK, "head"), P(BLK, None), P()),
        out_specs=P(BLK, "head"),
        check_vma=False,
    )
```

```python
import math

import jax
import jax.numpy as jnp
from jax import lax
from jax.experimental import pallas as pl
from jax.experimental.pallas import tpu as pltpu
from jax.sharding import Mesh
from jax.sharding import PartitionSpec as P

HEAD_DIM = 128
GROUP = 128
GROUPS = 128
AXES = ("z", "y", "xh", "core", "head")
BLK = AXES[:4]
MESH = pl.DeviceIdType.MESH
K_ROWS = 2 * GROUP + 16
CHUNK = K_ROWS + 2 * GROUP
Q_AT, Q_ROWS = CHUNK, 2 * GROUP + 16
NEG = -1e30
MASKED = -3e38
FAR = 1 << 20
TILE = 4
COEF = math.log2(math.e) / math.sqrt(HEAD_DIM)


def place():
    return tuple(lax.axis_index(a) for a in AXES)


def remote(src, dst, send, recv, to):
    return pltpu.make_async_remote_copy(
        src_ref=src, dst_ref=dst, send_sem=send, recv_sem=recv, device_id=to, device_id_type=MESH
    )


def spread_kernel(
    q_hbm, k_hbm, v_hbm, table_hbm, doc_hbm, kv_out, q_out, start_out, src, q_in, v_in, docs, table, loc, snd, own, yp, ym, rl, dd, qr
):
    z, y, xh, c, hd = place()
    up, down, over = lax.rem(y + 1, 4), lax.rem(y + 3, 4), lax.rem(y + 2, 4)
    zs = [z, lax.rem(z + 1, 4), lax.rem(z + 2, 4), lax.rem(z + 3, 4)]
    to_up, to_down, to_core = (z, up, xh, c, hd), (z, down, xh, c, hd), (z, y, xh, 1 - c, hd)
    local = [
        pltpu.make_async_copy(table_hbm, table, loc.at[0]),
        pltpu.make_async_copy(v_hbm, v_in, loc.at[1]),
        pltpu.make_async_copy(q_hbm, q_in, loc.at[2]),
        pltpu.make_async_copy(doc_hbm, docs, loc.at[3]),
    ]
    for h in range(4):
        keys_of_head = k_hbm.at[:, pl.ds(h * HEAD_DIM, HEAD_DIM)]
        local.append(pltpu.make_async_copy(keys_of_head, src.at[h, pl.ds(0, 2 * GROUP)], loc.at[4 + h]))
    for copy in local:
        copy.start()
    partners = [(zs[dz], y, xh, c, hd) for dz in (1, 2, 3)]
    partners += [(zs[dz], y, 1 - xh, c, hd) for dz in range(4)] + [to_up, to_down, to_core]
    barrier = pltpu.get_barrier_semaphore()
    for to in partners:
        pl.semaphore_signal(barrier, inc=1, device_id=to, device_id_type=MESH)

    local[0].wait()
    first = table[0, 0].astype(jnp.float32)
    for h in range(4):
        header = jnp.full((16, HEAD_DIM), first, jnp.float32).astype(jnp.bfloat16)
        src[h, K_ROWS - 16 : K_ROWS, :] = header
        src[h, Q_AT + 2 * GROUP :, :] = header
    local[1].wait()
    for h in range(4):
        for s in range(2):
            rows, cols = slice(s * GROUP, (s + 1) * GROUP), slice(h * HEAD_DIM, (h + 1) * HEAD_DIM)
            src[h, K_ROWS + s * GROUP : K_ROWS + (s + 1) * GROUP, :] = v_in[rows, cols].T
    for copy in local[2:]:
        copy.wait()
    pl.semaphore_wait(barrier, len(partners))

    sent = []

    def start(src_ref, dst_ref, recv, to):
        copy = remote(src_ref, dst_ref, snd.at[len(sent)], recv, to)
        copy.start()
        sent.append(copy)

    def landed(dst_ref, recv):
        remote(dst_ref, dst_ref, snd.at[0], recv, to_core).wait_recv()

    span = (pl.ds(0, K_ROWS), pl.ds(K_ROWS, 2 * GROUP))

    def piece(zz, yy, cc, p):
        return kv_out.at[(zz * 4 + yy) * 2 + cc, span[p]]

    order = (0, 1, 3, 2)
    came = [zs[(4 - dz) % 4] for dz in order]

    def first_hop(s, p):
        mine = piece(came[s], y, c, p)
        here = src.at[z, span[p]]
        if s > 0:
            landed(mine, own.at[s, p])
            here = mine
        start(here, mine, yp.at[s, p], to_up)
        start(here, mine, ym.at[s, p], to_down)
        start(here, mine, dd.at[s, 0, p], to_core)

    def second_hop(s, p):
        below, above = piece(came[s], down, c, p), piece(came[s], up, c, p)
        landed(below, yp.at[s, p])
        if p == 0:
            start(below, below, rl.at[s, p], to_up)
        start(below, below, dd.at[s, 1, p], to_core)
        landed(above, ym.at[s, p])
        if p == 1:
            start(above, above, rl.at[s, p], to_down)
        start(above, above, dd.at[s, 2, p], to_core)

    def last_hop(s, p):
        across = piece(came[s], over, c, p)
        landed(across, rl.at[s, p])
        start(across, across, dd.at[s, 3, p], to_core)

    first_hop(0, 0)
    for s, p in ((1, 0), (2, 0), (1, 1), (2, 1), (3, 0), (3, 1)):
        dz = order[s]
        start(src.at[zs[dz], span[p]], piece(z, y, c, p), own.at[s, p], (zs[dz], y, xh, c, hd))
    first_hop(0, 1)
    kv_out[(z * 4 + y) * 2 + c] = src[z, 0:CHUNK]
    for h in range(4):
        for s in range(2):
            rows, cols = slice(s * GROUP, (s + 1) * GROUP), slice(h * HEAD_DIM, (h + 1) * HEAD_DIM)
            src[h, Q_AT + s * GROUP : Q_AT + (s + 1) * GROUP, :] = q_in[rows, cols].T
    held = docs[...]
    for d in range(16):
        counted = jnp.sum(jnp.where(held < d, 1, 0), axis=0, keepdims=True)
        start_out[d : d + 1, :] = jnp.broadcast_to(jnp.sum(counted, axis=1, keepdims=True), (1, 128))
    q_span, q_mine = pl.ds(Q_AT, Q_ROWS), q_out.at[z * 2 + xh]
    q_out[z * 2 + xh] = src[z, Q_AT:]
    for dz in (1, 3, 2, 0):
        for dx in (1, 0):
            if dz or dx:
                start(src.at[zs[dz], q_span], q_mine, qr.at[dz * 2 + dx], (zs[dz], y, 1 - xh if dx else xh, c, hd))
    for s in range(1, 4):
        for p in range(2):
            first_hop(s, p)
            second_hop(s - 1, p)
            if s > 1:
                last_hop(s - 2, p)
    for p in range(2):
        second_hop(3, p)
        last_hop(2, p)
    for p in range(2):
        last_hop(3, p)

    for dz in range(4):
        for dx in range(2):
            if dz or dx:
                landed(q_out.at[zs[(4 - dz) % 4] * 2 + (1 - xh if dx else xh)], qr.at[dz * 2 + dx])
    for s in range(4):
        for i, yy in enumerate((y, down, up, over)):
            for p in range(2):
                landed(piece(came[s], yy, 1 - c, p), dd.at[s, i, p])
    for copy in sent:
        copy.wait_send()


def attend_kernel(kv, q, start_ref, o_ref, l_ref, plan, sm, low_s, bias_s, top_s, weight_s, acc_s, s_even, s_odd, sem):
    lane = lax.broadcasted_iota(jnp.int32, (1, 128), 1)
    lane32 = lax.broadcasted_iota(jnp.int32, (32, 128), 1)
    lane16 = lax.broadcasted_iota(jnp.int32, (16, 128), 1)
    code = lax.broadcasted_iota(jnp.int32, (32, 128), 0) * 2
    first = kv[:, 2 * GROUP, :].astype(jnp.float32).astype(jnp.int32)
    second = GROUPS - 1 - first
    at = jnp.where(first == lane32, code + 1, 0) + jnp.where(second == lane32, code + 2, 0)
    inv = jnp.sum(at, axis=0, keepdims=True) - 1
    here = jnp.where(inv >= 0, 1, 0)
    rank0 = jnp.sum(jnp.where(lane32 < first, here, 0), axis=1, keepdims=True)
    rank1 = jnp.sum(jnp.where(lane32 < second, here, 0), axis=1, keepdims=True)
    listed = jnp.where(rank0 == lane32, code * GROUPS, 0) + jnp.where(rank1 == lane32, (code + 1) * GROUPS, 0)
    plan[0:1, :] = jnp.sum(listed, axis=0, keepdims=True)
    plan[1:2, :] = inv

    q_first = q[:, 2 * GROUP, :].astype(jnp.float32).astype(jnp.int32)
    group = jnp.concatenate([q_first, GROUPS - 1 - q_first], axis=0)
    q_pos = group * GROUP + lane16
    low, low_first = jnp.zeros_like(q_pos), jnp.zeros_like(q_pos)
    for d in range(1, 16):
        begin = start_ref[d : d + 1, :]
        low = jnp.where(begin <= q_pos, begin, low)
        low_first = jnp.where(begin <= group * GROUP, begin, low_first)
    low_s[...] = low
    bias_s[...] = jnp.where(low == low_first, 0.0, MASKED)
    low_group = lax.shift_right_logical(low_first, 7)
    plan[16:32, :] = group
    plan[32:48, :] = low_group
    begin_at = jnp.sum(jnp.where(lane16 <= low_group, here, 0), axis=1, keepdims=True)
    end_at = jnp.sum(jnp.where(lane16 < group, here, 0), axis=1, keepdims=True)
    tiles = lax.shift_right_logical(jnp.maximum(end_at - begin_at, 0) + (TILE - 1), 2)
    begin_at, end_at, tiles = (jnp.broadcast_to(x, (16, 128)) for x in (begin_at, end_at, tiles))
    done = jnp.zeros((1, 128), jnp.int32)
    item = [lane, lane + 128, lane + 256]
    item_u, item_at, item_end = [[jnp.zeros((1, 128), jnp.int32) for _ in item] for _ in range(3)]
    for u in range(16):
        after = done + tiles[u : u + 1, :]
        for i, n in enumerate(item):
            mine = (done <= n) & (n < after)
            item_u[i] = jnp.where(mine, u, item_u[i])
            item_at[i] = jnp.where(mine, begin_at[u : u + 1, :] + (n - done) * TILE, item_at[i])
            item_end[i] = jnp.where(mine, end_at[u : u + 1, :], item_end[i])
        done = after
    for i in range(3):
        plan[2 + i : 3 + i, :] = item_u[i]
        plan[5 + i : 6 + i, :] = item_at[i]
        plan[8 + i : 9 + i, :] = item_end[i]
    plan[11:12, :] = done
    copy = pltpu.make_async_copy(plan, sm, sem)
    copy.start()
    copy.wait()

    row = lax.broadcasted_iota(jnp.int32, (GROUP, GROUP), 0)

    def half(slot, base):
        return pl.ds(pl.multiple_of(base + lax.rem(slot, 2) * GROUP, 16), GROUP)

    def queries_of(u):
        return q[lax.rem(u, 8), pl.ds(pl.multiple_of(lax.div(u, 8) * GROUP, GROUP), GROUP), :]

    def edges(u):
        g, low_g = sm[16 + u, 0], sm[32 + u, 0]
        q_t = queries_of(u)
        lower = low_s[pl.ds(u, 1), :]
        upper = g * GROUP + lane
        scores, held = [], []
        for key_group, wanted in ((g, True), (low_g, low_g < g)):
            found = sm[1, key_group]
            slot = jnp.maximum(found, 0)
            base = jnp.where((found >= 0) & wanted, key_group * GROUP, FAR)
            one = jnp.dot(kv[lax.div(slot, 2), half(slot, 0), :], q_t, preferred_element_type=jnp.float32)
            seen = (row >= lower - base) & (row <= upper - base)
            scores.append(jnp.where(seen, one, MASKED))
            held.append(kv[lax.div(slot, 2), half(slot, K_ROWS), :])
        top = jnp.full((1, GROUP), NEG, jnp.float32)
        for one in scores:
            top = jnp.maximum(top, jnp.max(one, axis=0, keepdims=True))
        parts = [jnp.exp2((one - top) * COEF) for one in scores]
        top_s[pl.ds(u, 1), :] = top
        weight_s[pl.ds(u, 1), :] = sum(jnp.sum(part, axis=0, keepdims=True) for part in parts)
        acc_s[u] = jnp.dot(
            jnp.concatenate(held, axis=1),
            jnp.concatenate([part.astype(jnp.bfloat16) for part in parts], axis=0),
            preferred_element_type=jnp.float32,
        )

    @pl.loop(0, 8)
    def _(k):
        edges(2 * k)
        edges(2 * k + 1)

    def read(i):
        r, k = lax.shift_right_logical(i, 7), lax.bitwise_and(i, 127)
        return sm[2 + r, k], sm[5 + r, k], sm[8 + r, k]

    def slot_of(e, end):
        return lax.shift_right_logical(sm[0, jnp.maximum(jnp.minimum(e, end - 1), 0)], 7)

    def score(i, dst):
        u, e, end = read(i)
        q_t = queries_of(u)
        for j in range(TILE):
            slot = slot_of(e + j, end)
            dst[j * GROUP : (j + 1) * GROUP, :] = jnp.dot(
                kv[lax.div(slot, 2), half(slot, 0), :], q_t, preferred_element_type=jnp.float32
            )

    def absorb(i, src):
        u, e, end = read(i)
        lanes = bias_s[pl.ds(u, 1), :]
        top = top_s[pl.ds(u, 1), :]
        new_top, biases, held, parts = top, [], [], []
        for j in range(TILE):
            biases.append(jnp.where(e + j < end, lanes, MASKED))
            best = jnp.max(src[j * GROUP : (j + 1) * GROUP, :], axis=0, keepdims=True)
            new_top = jnp.maximum(new_top, best + biases[j])
        factor = jnp.exp2((top - new_top) * COEF)
        weight = weight_s[pl.ds(u, 1), :] * factor
        for j in range(TILE):
            part = jnp.exp2((src[j * GROUP : (j + 1) * GROUP, :] - (new_top - biases[j])) * COEF)
            weight = weight + jnp.sum(part, axis=0, keepdims=True)
            parts.append(part.astype(jnp.bfloat16))
            slot = slot_of(e + j, end)
            held.append(kv[lax.div(slot, 2), half(slot, K_ROWS), :])
        top_s[pl.ds(u, 1), :] = new_top
        weight_s[pl.ds(u, 1), :] = weight
        acc_s[u] = acc_s[u] * factor + jnp.dot(
            jnp.concatenate(held, axis=1), jnp.concatenate(parts, axis=0), preferred_element_type=jnp.float32
        )

    total = sm[11, 0]
    score(jnp.int32(0), s_even)

    @pl.loop(0, lax.shift_right_logical(total + 1, 1))
    def _(k):
        i = 2 * k
        score(i + 1, s_odd)
        absorb(i, s_even)
        score(i + 2, s_even)
        absorb(i + 1, s_odd)

    @pl.loop(0, 16)
    def _(u):
        weight = weight_s[pl.ds(u, 1), :]
        some = weight > 0.0
        safe = jnp.where(some, weight, 1.0)
        ch, s = lax.rem(u, 8), lax.div(u, 8)
        o_ref[ch, pl.ds(pl.multiple_of(s * GROUP, GROUP), GROUP), :] = (acc_s[u] * (1.0 / safe)).astype(jnp.bfloat16)
        l_ref[ch, pl.ds(s, 1), :] = jnp.where(some, top_s[pl.ds(u, 1), :] * COEF + jnp.log2(safe), NEG)


def merge_kernel(o_ref, l_ref, out_ref, o_in, l_in, snd, orecv, lrecv):
    z, y, xh, c, hd = place()
    zs = [z, lax.rem(z + 1, 4), lax.rem(z + 2, 4), lax.rem(z + 3, 4)]
    peers = [(dz, dx) for dz in (2, 1, 3, 0) for dx in (1, 0) if dz or dx]
    barrier = pltpu.get_barrier_semaphore()
    for dz, dx in peers:
        to = (zs[dz], y, 1 - xh if dx else xh, c, hd)
        pl.semaphore_signal(barrier, inc=1, device_id=to, device_id_type=MESH)
    mine = z * 2 + xh
    o_in[mine] = o_ref[mine]
    l_in[mine] = l_ref[mine]
    pl.semaphore_wait(barrier, len(peers))
    sent = []
    for n, (dz, dx) in enumerate(peers):
        side = 1 - xh if dx else xh
        to, theirs = (zs[dz], y, side, c, hd), zs[dz] * 2 + side
        for src, dst, recv in ((o_ref, o_in, orecv), (l_ref, l_in, lrecv)):
            copy = remote(src.at[theirs], dst.at[mine], snd.at[len(sent)], recv.at[dz * 2 + dx], to)
            copy.start()
            sent.append(copy)
    for dz, dx in peers:
        side = 1 - xh if dx else xh
        theirs = zs[(4 - dz) % 4] * 2 + side
        to = (zs[1], y, xh, c, hd)
        remote(o_ref.at[0], o_in.at[theirs], snd.at[0], orecv.at[dz * 2 + dx], to).wait_recv()
        remote(l_ref.at[0], l_in.at[theirs], snd.at[0], lrecv.at[dz * 2 + dx], to).wait_recv()
    for h in range(4):
        for s in range(2):
            rows = slice(s * GROUP, (s + 1) * GROUP)
            a, b = l_in[2 * h, s : s + 1, :], l_in[2 * h + 1, s : s + 1, :]
            most = jnp.maximum(a, b)
            wa, wb = jnp.exp2(a - most), jnp.exp2(b - most)
            total = wa + wb
            merged = o_in[2 * h, rows, :].astype(jnp.float32) * (wa / total)
            merged = merged + o_in[2 * h + 1, rows, :].astype(jnp.float32) * (wb / total)
            out_ref[rows, h * HEAD_DIM : (h + 1) * HEAD_DIM] = merged.T.astype(jnp.bfloat16)
    for copy in sent:
        copy.wait_send()


def shards(queries, keys, values, group_table, doc_ids):
    vmem = pl.BlockSpec(memory_space=pltpu.VMEM)
    hbm = pl.BlockSpec(memory_space=pltpu.HBM)
    dma = pltpu.SemaphoreType.DMA
    kv, q, begins = pl.pallas_call(
        spread_kernel,
        out_shape=(
            pltpu.VMEM((32, CHUNK, HEAD_DIM), jnp.bfloat16),
            pltpu.VMEM((8, Q_ROWS, HEAD_DIM), jnp.bfloat16),
            pltpu.VMEM((16, 128), jnp.int32),
        ),
        in_specs=[hbm] * 5,
        out_specs=(vmem, vmem, vmem),
        scratch_shapes=[
            pltpu.VMEM((4, Q_AT + Q_ROWS, HEAD_DIM), jnp.bfloat16),
            pltpu.VMEM(queries.shape, jnp.bfloat16),
            pltpu.VMEM(values.shape, jnp.bfloat16),
            pltpu.VMEM((128, 128), jnp.int32),
            pltpu.SMEM((1, 2), jnp.int32),
            dma((8,)), dma((69,)), dma((4, 2)), dma((4, 2)), dma((4, 2)), dma((4, 2)), dma((4, 4, 2)), dma((8,)),
        ],
        compiler_params=pltpu.CompilerParams(collective_id=0, has_side_effects=True, vmem_limit_bytes=62050000),
    )(queries, keys, values, group_table, doc_ids.reshape(128, 128))
    o, l = pl.pallas_call(
        attend_kernel,
        out_shape=(
            pltpu.VMEM((8, 2 * GROUP, HEAD_DIM), jnp.bfloat16),
            pltpu.VMEM((8, 8, GROUP), jnp.float32),
        ),
        in_specs=[vmem, vmem, vmem],
        out_specs=(vmem, vmem),
        scratch_shapes=[
            pltpu.VMEM((48, 128), jnp.int32),
            pltpu.SMEM((48, 128), jnp.int32),
            pltpu.VMEM((16, 128), jnp.int32),
            pltpu.VMEM((16, 128), jnp.float32),
            pltpu.VMEM((16, 128), jnp.float32),
            pltpu.VMEM((16, 128), jnp.float32),
            pltpu.VMEM((16, HEAD_DIM, GROUP), jnp.float32),
            pltpu.VMEM((TILE * GROUP, GROUP), jnp.float32),
            pltpu.VMEM((TILE * GROUP, GROUP), jnp.float32),
            dma,
        ],
        compiler_params=pltpu.CompilerParams(vmem_limit_bytes=16 << 20),
    )(kv, q, begins)
    return pl.pallas_call(
        merge_kernel,
        out_shape=jax.ShapeDtypeStruct(queries.shape, jnp.bfloat16),
        in_specs=[vmem, vmem],
        out_specs=vmem,
        scratch_shapes=[
            pltpu.VMEM((8, 2 * GROUP, HEAD_DIM), jnp.bfloat16),
            pltpu.VMEM((8, 8, GROUP), jnp.float32),
            dma((14,)), dma((8,)), dma((8,)),
        ],
        compiler_params=pltpu.CompilerParams(collective_id=1, has_side_effects=True, vmem_limit_bytes=16 << 20),
    )(o, l)


def solution(mesh):
    split = Mesh(mesh.devices.reshape(4, 4, 2, 2, mesh.shape["head"]), AXES)
    return jax.shard_map(
        shards,
        mesh=split,
        in_specs=(P(BLK, "head"), P(BLK, "head"), P(BLK, "head"), P(BLK, None), P()),
        out_specs=P(BLK, "head"),
        check_vma=False,
    )
```

```python
import math

import jax
import jax.numpy as jnp
from jax import lax
from jax.experimental import pallas as pl
from jax.experimental.pallas import tpu as pltpu
from jax.sharding import Mesh
from jax.sharding import PartitionSpec as P

HEAD_DIM = 128
GROUP = 128
GROUPS = 128
AXES = ("z", "y", "xh", "core", "head")
BLK = AXES[:4]
MESH = pl.DeviceIdType.MESH
K_ROWS = 2 * GROUP + 16
CHUNK = K_ROWS + 2 * GROUP
Q_AT, Q_ROWS = CHUNK, 2 * GROUP + 16
NEG = -1e30
MASKED = -3e38
FAR = 1 << 20
TILE = 4
COEF = math.log2(math.e) / math.sqrt(HEAD_DIM)


def place():
    return tuple(lax.axis_index(a) for a in AXES)


def remote(src, dst, send, recv, to):
    return pltpu.make_async_remote_copy(
        src_ref=src, dst_ref=dst, send_sem=send, recv_sem=recv, device_id=to, device_id_type=MESH
    )


def spread_kernel(
    q_hbm, k_hbm, v_hbm, table_hbm, doc_hbm, kv_out, q_out, start_out, src, q_in, v_in, docs, table, loc, snd, own, yp, ym, rl, dd, qr
):
    z, y, xh, c, hd = place()
    up, down, over = lax.rem(y + 1, 4), lax.rem(y + 3, 4), lax.rem(y + 2, 4)
    zs = [z, lax.rem(z + 1, 4), lax.rem(z + 2, 4), lax.rem(z + 3, 4)]
    to_up, to_down, to_core = (z, up, xh, c, hd), (z, down, xh, c, hd), (z, y, xh, 1 - c, hd)
    local = [
        pltpu.make_async_copy(table_hbm, table, loc.at[0]),
        pltpu.make_async_copy(v_hbm, v_in, loc.at[1]),
        pltpu.make_async_copy(q_hbm, q_in, loc.at[2]),
        pltpu.make_async_copy(doc_hbm, docs, loc.at[3]),
    ]
    for h in range(4):
        keys_of_head = k_hbm.at[:, pl.ds(h * HEAD_DIM, HEAD_DIM)]
        local.append(pltpu.make_async_copy(keys_of_head, src.at[h, pl.ds(0, 2 * GROUP)], loc.at[4 + h]))
    for copy in local:
        copy.start()
    partners = [(zs[dz], y, xh, c, hd) for dz in (1, 2, 3)]
    partners += [(zs[dz], y, 1 - xh, c, hd) for dz in range(4)] + [to_up, to_down, to_core]
    barrier = pltpu.get_barrier_semaphore()
    for to in partners:
        pl.semaphore_signal(barrier, inc=1, device_id=to, device_id_type=MESH)

    local[0].wait()
    first = table[0, 0].astype(jnp.float32)
    for h in range(4):
        header = jnp.full((16, HEAD_DIM), first, jnp.float32).astype(jnp.bfloat16)
        src[h, K_ROWS - 16 : K_ROWS, :] = header
        src[h, Q_AT + 2 * GROUP :, :] = header
    local[1].wait()
    for h in range(4):
        for s in range(2):
            rows, cols = slice(s * GROUP, (s + 1) * GROUP), slice(h * HEAD_DIM, (h + 1) * HEAD_DIM)
            src[h, K_ROWS + s * GROUP : K_ROWS + (s + 1) * GROUP, :] = v_in[rows, cols].T
    for copy in local[2:]:
        copy.wait()
    pl.semaphore_wait(barrier, len(partners))

    sent = []

    def start(src_ref, dst_ref, recv, to):
        copy = remote(src_ref, dst_ref, snd.at[len(sent)], recv, to)
        copy.start()
        sent.append(copy)

    def landed(dst_ref, recv):
        remote(dst_ref, dst_ref, snd.at[0], recv, to_core).wait_recv()

    span = (pl.ds(0, K_ROWS), pl.ds(K_ROWS, 2 * GROUP))

    def piece(zz, yy, cc, p):
        return kv_out.at[(zz * 4 + yy) * 2 + cc, span[p]]

    order = (0, 1, 3, 2)
    came = [zs[(4 - dz) % 4] for dz in order]

    def first_hop(s, p):
        mine = piece(came[s], y, c, p)
        here = src.at[z, span[p]]
        if s > 0:
            landed(mine, own.at[s, p])
            here = mine
        start(here, mine, yp.at[s, p], to_up)
        start(here, mine, ym.at[s, p], to_down)
        start(here, mine, dd.at[s, 0, p], to_core)

    def second_hop(s, p):
        below, above = piece(came[s], down, c, p), piece(came[s], up, c, p)
        landed(below, yp.at[s, p])
        if p == 0:
            start(below, below, rl.at[s, p], to_up)
        start(below, below, dd.at[s, 1, p], to_core)
        landed(above, ym.at[s, p])
        if p == 1:
            start(above, above, rl.at[s, p], to_down)
        start(above, above, dd.at[s, 2, p], to_core)

    def last_hop(s, p):
        across = piece(came[s], over, c, p)
        landed(across, rl.at[s, p])
        start(across, across, dd.at[s, 3, p], to_core)

    first_hop(0, 0)
    for s, p in ((1, 0), (2, 0), (1, 1), (2, 1), (3, 0), (3, 1)):
        dz = order[s]
        start(src.at[zs[dz], span[p]], piece(z, y, c, p), own.at[s, p], (zs[dz], y, xh, c, hd))
    first_hop(0, 1)
    kv_out[(z * 4 + y) * 2 + c] = src[z, 0:CHUNK]
    for h in range(4):
        for s in range(2):
            rows, cols = slice(s * GROUP, (s + 1) * GROUP), slice(h * HEAD_DIM, (h + 1) * HEAD_DIM)
            src[h, Q_AT + s * GROUP : Q_AT + (s + 1) * GROUP, :] = q_in[rows, cols].T
    held = docs[...]
    for d in range(16):
        counted = jnp.sum(jnp.where(held < d, 1, 0), axis=0, keepdims=True)
        start_out[d : d + 1, :] = jnp.broadcast_to(jnp.sum(counted, axis=1, keepdims=True), (1, 128))
    q_span, q_mine = pl.ds(Q_AT, Q_ROWS), q_out.at[z * 2 + xh]
    q_out[z * 2 + xh] = src[z, Q_AT:]
    for dz in (1, 3, 2, 0):
        for dx in (1, 0):
            if dz or dx:
                start(src.at[zs[dz], q_span], q_mine, qr.at[dz * 2 + dx], (zs[dz], y, 1 - xh if dx else xh, c, hd))
    for s in range(1, 4):
        for p in range(2):
            first_hop(s, p)
            second_hop(s - 1, p)
            if s > 1:
                last_hop(s - 2, p)
    for p in range(2):
        second_hop(3, p)
        last_hop(2, p)
    for p in range(2):
        last_hop(3, p)

    for dz in range(4):
        for dx in range(2):
            if dz or dx:
                landed(q_out.at[zs[(4 - dz) % 4] * 2 + (1 - xh if dx else xh)], qr.at[dz * 2 + dx])
    for s in range(4):
        for i, yy in enumerate((y, down, up, over)):
            for p in range(2):
                landed(piece(came[s], yy, 1 - c, p), dd.at[s, i, p])
    for copy in sent:
        copy.wait_send()


def attend_kernel(kv, q, start_ref, o_ref, l_ref, plan, sm, low_s, bias_s, top_s, weight_s, acc_s, s_even, s_odd, sem):
    lane = lax.broadcasted_iota(jnp.int32, (1, 128), 1)
    lane32 = lax.broadcasted_iota(jnp.int32, (32, 128), 1)
    lane16 = lax.broadcasted_iota(jnp.int32, (16, 128), 1)
    code = lax.broadcasted_iota(jnp.int32, (32, 128), 0) * 2
    first = kv[:, 2 * GROUP, :].astype(jnp.float32).astype(jnp.int32)
    second = GROUPS - 1 - first
    at = jnp.where(first == lane32, code + 1, 0) + jnp.where(second == lane32, code + 2, 0)
    inv = jnp.sum(at, axis=0, keepdims=True) - 1
    here = jnp.where(inv >= 0, 1, 0)
    rank0 = jnp.sum(jnp.where(lane32 < first, here, 0), axis=1, keepdims=True)
    rank1 = jnp.sum(jnp.where(lane32 < second, here, 0), axis=1, keepdims=True)
    listed = jnp.where(rank0 == lane32, code * GROUPS, 0) + jnp.where(rank1 == lane32, (code + 1) * GROUPS, 0)
    plan[0:1, :] = jnp.sum(listed, axis=0, keepdims=True)
    plan[1:2, :] = inv

    q_first = q[:, 2 * GROUP, :].astype(jnp.float32).astype(jnp.int32)
    group = jnp.concatenate([q_first, GROUPS - 1 - q_first], axis=0)
    q_pos = group * GROUP + lane16
    low, low_first = jnp.zeros_like(q_pos), jnp.zeros_like(q_pos)
    for d in range(1, 16):
        begin = start_ref[d : d + 1, :]
        low = jnp.where(begin <= q_pos, begin, low)
        low_first = jnp.where(begin <= group * GROUP, begin, low_first)
    low_s[...] = low
    bias_s[...] = jnp.where(low == low_first, 0.0, MASKED)
    low_group = lax.shift_right_logical(low_first, 7)
    plan[16:32, :] = group
    plan[32:48, :] = low_group
    begin_at = jnp.sum(jnp.where(lane16 <= low_group, here, 0), axis=1, keepdims=True)
    end_at = jnp.sum(jnp.where(lane16 < group, here, 0), axis=1, keepdims=True)
    tiles = lax.shift_right_logical(jnp.maximum(end_at - begin_at, 0) + (TILE - 1), 2)
    begin_at, end_at, tiles = (jnp.broadcast_to(x, (16, 128)) for x in (begin_at, end_at, tiles))
    done = jnp.zeros((1, 128), jnp.int32)
    item = [lane, lane + 128, lane + 256]
    item_u, item_at, item_end = [[jnp.zeros((1, 128), jnp.int32) for _ in item] for _ in range(3)]
    for u in range(16):
        after = done + tiles[u : u + 1, :]
        for i, n in enumerate(item):
            mine = (done <= n) & (n < after)
            item_u[i] = jnp.where(mine, u, item_u[i])
            item_at[i] = jnp.where(mine, begin_at[u : u + 1, :] + (n - done) * TILE, item_at[i])
            item_end[i] = jnp.where(mine, end_at[u : u + 1, :], item_end[i])
        done = after
    for i in range(3):
        plan[2 + i : 3 + i, :] = item_u[i]
        plan[5 + i : 6 + i, :] = item_at[i]
        plan[8 + i : 9 + i, :] = item_end[i]
    plan[11:12, :] = done
    copy = pltpu.make_async_copy(plan, sm, sem)
    copy.start()
    copy.wait()

    row = lax.broadcasted_iota(jnp.int32, (GROUP, GROUP), 0)

    def half(slot, base):
        return pl.ds(pl.multiple_of(base + lax.rem(slot, 2) * GROUP, 16), GROUP)

    def queries_of(u):
        return q[lax.rem(u, 8), pl.ds(pl.multiple_of(lax.div(u, 8) * GROUP, GROUP), GROUP), :]

    def edges(u):
        g, low_g = sm[16 + u, 0], sm[32 + u, 0]
        q_t = queries_of(u)
        lower = low_s[pl.ds(u, 1), :]
        upper = g * GROUP + lane
        scores, held = [], []
        for key_group, wanted in ((g, True), (low_g, low_g < g)):
            found = sm[1, key_group]
            slot = jnp.maximum(found, 0)
            base = jnp.where((found >= 0) & wanted, key_group * GROUP, FAR)
            one = jnp.dot(kv[lax.div(slot, 2), half(slot, 0), :], q_t, preferred_element_type=jnp.float32)
            seen = (row >= lower - base) & (row <= upper - base)
            scores.append(jnp.where(seen, one, MASKED))
            held.append(kv[lax.div(slot, 2), half(slot, K_ROWS), :])
        top = jnp.full((1, GROUP), NEG, jnp.float32)
        for one in scores:
            top = jnp.maximum(top, jnp.max(one, axis=0, keepdims=True))
        parts = [jnp.exp2((one - top) * COEF) for one in scores]
        top_s[pl.ds(u, 1), :] = top
        weight_s[pl.ds(u, 1), :] = sum(jnp.sum(part, axis=0, keepdims=True) for part in parts)
        acc_s[u] = jnp.dot(
            jnp.concatenate(held, axis=1),
            jnp.concatenate([part.astype(jnp.bfloat16) for part in parts], axis=0),
            preferred_element_type=jnp.float32,
        )

    @pl.loop(0, 4)
    def _(k):
        for n in range(4):
            edges(4 * k + n)

    def read(i):
        r, k = lax.shift_right_logical(i, 7), lax.bitwise_and(i, 127)
        return sm[2 + r, k], sm[5 + r, k], sm[8 + r, k]

    def slot_of(e, end):
        return lax.shift_right_logical(sm[0, jnp.maximum(jnp.minimum(e, end - 1), 0)], 7)

    def score(i, dst):
        u, e, end = read(i)
        q_t = queries_of(u)
        for j in range(TILE):
            slot = slot_of(e + j, end)
            dst[j * GROUP : (j + 1) * GROUP, :] = jnp.dot(
                kv[lax.div(slot, 2), half(slot, 0), :], q_t, preferred_element_type=jnp.float32
            )

    def absorb(i, src):
        u, e, end = read(i)
        lanes = bias_s[pl.ds(u, 1), :]
        top = top_s[pl.ds(u, 1), :]
        new_top, biases, held, parts = top, [], [], []
        for j in range(TILE):
            biases.append(jnp.where(e + j < end, lanes, MASKED))
            best = jnp.max(src[j * GROUP : (j + 1) * GROUP, :], axis=0, keepdims=True)
            new_top = jnp.maximum(new_top, best + biases[j])
        factor = jnp.exp2((top - new_top) * COEF)
        weight = weight_s[pl.ds(u, 1), :] * factor
        for j in range(TILE):
            part = jnp.exp2((src[j * GROUP : (j + 1) * GROUP, :] - (new_top - biases[j])) * COEF)
            weight = weight + jnp.sum(part, axis=0, keepdims=True)
            parts.append(part.astype(jnp.bfloat16))
            slot = slot_of(e + j, end)
            held.append(kv[lax.div(slot, 2), half(slot, K_ROWS), :])
        top_s[pl.ds(u, 1), :] = new_top
        weight_s[pl.ds(u, 1), :] = weight
        acc_s[u] = acc_s[u] * factor + jnp.dot(
            jnp.concatenate(held, axis=1), jnp.concatenate(parts, axis=0), preferred_element_type=jnp.float32
        )

    total = sm[11, 0]
    score(jnp.int32(0), s_even)

    @pl.loop(0, lax.shift_right_logical(total + 7, 3))
    def _(k):
        for n in range(0, 8, 2):
            i = 8 * k + n
            score(i + 1, s_odd)
            absorb(i, s_even)
            score(i + 2, s_even)
            absorb(i + 1, s_odd)

    @pl.loop(0, 16, unroll=4)
    def _(u):
        weight = weight_s[pl.ds(u, 1), :]
        some = weight > 0.0
        safe = jnp.where(some, weight, 1.0)
        ch, s = lax.rem(u, 8), lax.div(u, 8)
        o_ref[ch, pl.ds(pl.multiple_of(s * GROUP, GROUP), GROUP), :] = (acc_s[u] * (1.0 / safe)).astype(jnp.bfloat16)
        l_ref[ch, pl.ds(s, 1), :] = jnp.where(some, top_s[pl.ds(u, 1), :] * COEF + jnp.log2(safe), NEG)


def merge_kernel(o_ref, l_ref, out_ref, o_in, l_in, snd, orecv, lrecv):
    z, y, xh, c, hd = place()
    zs = [z, lax.rem(z + 1, 4), lax.rem(z + 2, 4), lax.rem(z + 3, 4)]
    peers = [(dz, dx) for dz in (2, 1, 3, 0) for dx in (1, 0) if dz or dx]
    barrier = pltpu.get_barrier_semaphore()
    for dz, dx in peers:
        to = (zs[dz], y, 1 - xh if dx else xh, c, hd)
        pl.semaphore_signal(barrier, inc=1, device_id=to, device_id_type=MESH)
    mine = z * 2 + xh
    o_in[mine] = o_ref[mine]
    l_in[mine] = l_ref[mine]
    pl.semaphore_wait(barrier, len(peers))
    sent = []
    for n, (dz, dx) in enumerate(peers):
        side = 1 - xh if dx else xh
        to, theirs = (zs[dz], y, side, c, hd), zs[dz] * 2 + side
        for src, dst, recv in ((o_ref, o_in, orecv), (l_ref, l_in, lrecv)):
            copy = remote(src.at[theirs], dst.at[mine], snd.at[len(sent)], recv.at[dz * 2 + dx], to)
            copy.start()
            sent.append(copy)
    for dz, dx in peers:
        side = 1 - xh if dx else xh
        theirs = zs[(4 - dz) % 4] * 2 + side
        to = (zs[1], y, xh, c, hd)
        remote(o_ref.at[0], o_in.at[theirs], snd.at[0], orecv.at[dz * 2 + dx], to).wait_recv()
        remote(l_ref.at[0], l_in.at[theirs], snd.at[0], lrecv.at[dz * 2 + dx], to).wait_recv()
    for h in range(4):
        for s in range(2):
            rows = slice(s * GROUP, (s + 1) * GROUP)
            a, b = l_in[2 * h, s : s + 1, :], l_in[2 * h + 1, s : s + 1, :]
            most = jnp.maximum(a, b)
            wa, wb = jnp.exp2(a - most), jnp.exp2(b - most)
            total = wa + wb
            merged = o_in[2 * h, rows, :].astype(jnp.float32) * (wa / total)
            merged = merged + o_in[2 * h + 1, rows, :].astype(jnp.float32) * (wb / total)
            out_ref[rows, h * HEAD_DIM : (h + 1) * HEAD_DIM] = merged.T.astype(jnp.bfloat16)
    for copy in sent:
        copy.wait_send()


def shards(queries, keys, values, group_table, doc_ids):
    vmem = pl.BlockSpec(memory_space=pltpu.VMEM)
    hbm = pl.BlockSpec(memory_space=pltpu.HBM)
    dma = pltpu.SemaphoreType.DMA
    kv, q, begins = pl.pallas_call(
        spread_kernel,
        out_shape=(
            pltpu.VMEM((32, CHUNK, HEAD_DIM), jnp.bfloat16),
            pltpu.VMEM((8, Q_ROWS, HEAD_DIM), jnp.bfloat16),
            pltpu.VMEM((16, 128), jnp.int32),
        ),
        in_specs=[hbm] * 5,
        out_specs=(vmem, vmem, vmem),
        scratch_shapes=[
            pltpu.VMEM((4, Q_AT + Q_ROWS, HEAD_DIM), jnp.bfloat16),
            pltpu.VMEM(queries.shape, jnp.bfloat16),
            pltpu.VMEM(values.shape, jnp.bfloat16),
            pltpu.VMEM((128, 128), jnp.int32),
            pltpu.SMEM((1, 2), jnp.int32),
            dma((8,)), dma((69,)), dma((4, 2)), dma((4, 2)), dma((4, 2)), dma((4, 2)), dma((4, 4, 2)), dma((8,)),
        ],
        compiler_params=pltpu.CompilerParams(collective_id=0, has_side_effects=True, vmem_limit_bytes=62050000),
    )(queries, keys, values, group_table, doc_ids.reshape(128, 128))
    o, l = pl.pallas_call(
        attend_kernel,
        out_shape=(
            pltpu.VMEM((8, 2 * GROUP, HEAD_DIM), jnp.bfloat16),
            pltpu.VMEM((8, 8, GROUP), jnp.float32),
        ),
        in_specs=[vmem, vmem, vmem],
        out_specs=(vmem, vmem),
        scratch_shapes=[
            pltpu.VMEM((48, 128), jnp.int32),
            pltpu.SMEM((48, 128), jnp.int32),
            pltpu.VMEM((16, 128), jnp.int32),
            pltpu.VMEM((16, 128), jnp.float32),
            pltpu.VMEM((16, 128), jnp.float32),
            pltpu.VMEM((16, 128), jnp.float32),
            pltpu.VMEM((16, HEAD_DIM, GROUP), jnp.float32),
            pltpu.VMEM((TILE * GROUP, GROUP), jnp.float32),
            pltpu.VMEM((TILE * GROUP, GROUP), jnp.float32),
            dma,
        ],
        compiler_params=pltpu.CompilerParams(vmem_limit_bytes=16 << 20),
    )(kv, q, begins)
    return pl.pallas_call(
        merge_kernel,
        out_shape=jax.ShapeDtypeStruct(queries.shape, jnp.bfloat16),
        in_specs=[vmem, vmem],
        out_specs=vmem,
        scratch_shapes=[
            pltpu.VMEM((8, 2 * GROUP, HEAD_DIM), jnp.bfloat16),
            pltpu.VMEM((8, 8, GROUP), jnp.float32),
            dma((14,)), dma((8,)), dma((8,)),
        ],
        compiler_params=pltpu.CompilerParams(collective_id=1, has_side_effects=True, vmem_limit_bytes=16 << 20),
    )(o, l)


def solution(mesh):
    split = Mesh(mesh.devices.reshape(4, 4, 2, 2, mesh.shape["head"]), AXES)
    return jax.shard_map(
        shards,
        mesh=split,
        in_specs=(P(BLK, "head"), P(BLK, "head"), P(BLK, "head"), P(BLK, None), P()),
        out_specs=P(BLK, "head"),
        check_vma=False,
    )
```

```python
import math

import jax
import jax.numpy as jnp
from jax import lax
from jax.experimental import pallas as pl
from jax.experimental.pallas import tpu as pltpu
from jax.sharding import Mesh
from jax.sharding import PartitionSpec as P

HEAD_DIM = 128
GROUP = 128
GROUPS = 128
AXES = ("z", "y", "xh", "core", "head")
BLK = AXES[:4]
MESH = pl.DeviceIdType.MESH
K_ROWS = 2 * GROUP + 16
CHUNK = K_ROWS + 2 * GROUP
Q_AT, Q_ROWS = CHUNK, 2 * GROUP + 16
NEG = -1e30
MASKED = -3e38
FAR = 1 << 20
TILE = 4
COEF = math.log2(math.e) / math.sqrt(HEAD_DIM)


def place():
    return tuple(lax.axis_index(a) for a in AXES)


def remote(src, dst, send, recv, to):
    return pltpu.make_async_remote_copy(
        src_ref=src, dst_ref=dst, send_sem=send, recv_sem=recv, device_id=to, device_id_type=MESH
    )


def spread_kernel(
    q_hbm, k_hbm, v_hbm, table_hbm, doc_hbm, kv_out, q_out, start_out, src, q_in, v_in, docs, table, loc, snd, own, yp, ym, rl, dd, qr
):
    z, y, xh, c, hd = place()
    up, down, over = lax.rem(y + 1, 4), lax.rem(y + 3, 4), lax.rem(y + 2, 4)
    zs = [z, lax.rem(z + 1, 4), lax.rem(z + 2, 4), lax.rem(z + 3, 4)]
    to_up, to_down, to_core = (z, up, xh, c, hd), (z, down, xh, c, hd), (z, y, xh, 1 - c, hd)
    local = [
        pltpu.make_async_copy(table_hbm, table, loc.at[0]),
        pltpu.make_async_copy(v_hbm, v_in, loc.at[1]),
        pltpu.make_async_copy(q_hbm, q_in, loc.at[2]),
        pltpu.make_async_copy(doc_hbm, docs, loc.at[3]),
    ]
    for h in range(4):
        keys_of_head = k_hbm.at[:, pl.ds(h * HEAD_DIM, HEAD_DIM)]
        local.append(pltpu.make_async_copy(keys_of_head, src.at[h, pl.ds(0, 2 * GROUP)], loc.at[4 + h]))
    for copy in local:
        copy.start()
    partners = [(zs[dz], y, xh, c, hd) for dz in (1, 2, 3)]
    partners += [(zs[dz], y, 1 - xh, c, hd) for dz in range(4)] + [to_up, to_down, to_core]
    barrier = pltpu.get_barrier_semaphore()
    for to in partners:
        pl.semaphore_signal(barrier, inc=1, device_id=to, device_id_type=MESH)

    local[0].wait()
    first = table[0, 0].astype(jnp.float32)
    for h in range(4):
        header = jnp.full((16, HEAD_DIM), first, jnp.float32).astype(jnp.bfloat16)
        src[h, K_ROWS - 16 : K_ROWS, :] = header
        src[h, Q_AT + 2 * GROUP :, :] = header
    local[1].wait()
    for h in range(4):
        for s in range(2):
            rows, cols = slice(s * GROUP, (s + 1) * GROUP), slice(h * HEAD_DIM, (h + 1) * HEAD_DIM)
            src[h, K_ROWS + s * GROUP : K_ROWS + (s + 1) * GROUP, :] = v_in[rows, cols].T
    for copy in local[2:]:
        copy.wait()
    pl.semaphore_wait(barrier, len(partners))

    sent = []

    def start(src_ref, dst_ref, recv, to):
        copy = remote(src_ref, dst_ref, snd.at[len(sent)], recv, to)
        copy.start()
        sent.append(copy)

    def landed(dst_ref, recv):
        remote(dst_ref, dst_ref, snd.at[0], recv, to_core).wait_recv()

    span = (pl.ds(0, K_ROWS), pl.ds(K_ROWS, 2 * GROUP))

    def piece(zz, yy, cc, p):
        return kv_out.at[(zz * 4 + yy) * 2 + cc, span[p]]

    order = (0, 1, 3, 2)
    came = [zs[(4 - dz) % 4] for dz in order]

    def first_hop(s, p):
        mine = piece(came[s], y, c, p)
        here = src.at[z, span[p]]
        if s > 0:
            landed(mine, own.at[s, p])
            here = mine
        start(here, mine, yp.at[s, p], to_up)
        start(here, mine, ym.at[s, p], to_down)
        start(here, mine, dd.at[s, 0, p], to_core)

    def second_hop(s, p):
        below, above = piece(came[s], down, c, p), piece(came[s], up, c, p)
        landed(below, yp.at[s, p])
        if p == 0:
            start(below, below, rl.at[s, p], to_up)
        start(below, below, dd.at[s, 1, p], to_core)
        landed(above, ym.at[s, p])
        if p == 1:
            start(above, above, rl.at[s, p], to_down)
        start(above, above, dd.at[s, 2, p], to_core)

    def last_hop(s, p):
        across = piece(came[s], over, c, p)
        landed(across, rl.at[s, p])
        start(across, across, dd.at[s, 3, p], to_core)

    first_hop(0, 0)
    for s, p in ((1, 0), (2, 0), (1, 1), (2, 1), (3, 0), (3, 1)):
        dz = order[s]
        start(src.at[zs[dz], span[p]], piece(z, y, c, p), own.at[s, p], (zs[dz], y, xh, c, hd))
    first_hop(0, 1)
    kv_out[(z * 4 + y) * 2 + c] = src[z, 0:CHUNK]
    for h in range(4):
        for s in range(2):
            rows, cols = slice(s * GROUP, (s + 1) * GROUP), slice(h * HEAD_DIM, (h + 1) * HEAD_DIM)
            src[h, Q_AT + s * GROUP : Q_AT + (s + 1) * GROUP, :] = q_in[rows, cols].T
    held = docs[...]
    for d in range(16):
        counted = jnp.sum(jnp.where(held < d, 1, 0), axis=0, keepdims=True)
        start_out[d : d + 1, :] = jnp.broadcast_to(jnp.sum(counted, axis=1, keepdims=True), (1, 128))
    q_span, q_mine = pl.ds(Q_AT, Q_ROWS), q_out.at[z * 2 + xh]
    q_out[z * 2 + xh] = src[z, Q_AT:]
    def send_queries():
        for dz in (1, 3, 2, 0):
            for dx in (1, 0):
                if dz or dx:
                    start(src.at[zs[dz], q_span], q_mine, qr.at[dz * 2 + dx], (zs[dz], y, 1 - xh if dx else xh, c, hd))

    for s in range(1, 4):
        for p in range(2):
            first_hop(s, p)
            second_hop(s - 1, p)
            if s > 1:
                last_hop(s - 2, p)
        if s == 2:
            send_queries()
    for p in range(2):
        second_hop(3, p)
        last_hop(2, p)
    for p in range(2):
        last_hop(3, p)

    for dz in range(4):
        for dx in range(2):
            if dz or dx:
                landed(q_out.at[zs[(4 - dz) % 4] * 2 + (1 - xh if dx else xh)], qr.at[dz * 2 + dx])
    for s in range(4):
        for i, yy in enumerate((y, down, up, over)):
            for p in range(2):
                landed(piece(came[s], yy, 1 - c, p), dd.at[s, i, p])
    for copy in sent:
        copy.wait_send()


def attend_kernel(kv, q, start_ref, o_ref, l_ref, plan, sm, low_s, bias_s, top_s, weight_s, acc_s, s_even, s_odd, sem):
    lane = lax.broadcasted_iota(jnp.int32, (1, 128), 1)
    lane32 = lax.broadcasted_iota(jnp.int32, (32, 128), 1)
    lane16 = lax.broadcasted_iota(jnp.int32, (16, 128), 1)
    code = lax.broadcasted_iota(jnp.int32, (32, 128), 0) * 2
    first = kv[:, 2 * GROUP, :].astype(jnp.float32).astype(jnp.int32)
    second = GROUPS - 1 - first
    at = jnp.where(first == lane32, code + 1, 0) + jnp.where(second == lane32, code + 2, 0)
    inv = jnp.sum(at, axis=0, keepdims=True) - 1
    here = jnp.where(inv >= 0, 1, 0)
    rank0 = jnp.sum(jnp.where(lane32 < first, here, 0), axis=1, keepdims=True)
    rank1 = jnp.sum(jnp.where(lane32 < second, here, 0), axis=1, keepdims=True)
    listed = jnp.where(rank0 == lane32, code * GROUPS, 0) + jnp.where(rank1 == lane32, (code + 1) * GROUPS, 0)
    plan[0:1, :] = jnp.sum(listed, axis=0, keepdims=True)
    plan[1:2, :] = inv

    q_first = q[:, 2 * GROUP, :].astype(jnp.float32).astype(jnp.int32)
    group = jnp.concatenate([q_first, GROUPS - 1 - q_first], axis=0)
    q_pos = group * GROUP + lane16
    low, low_first = jnp.zeros_like(q_pos), jnp.zeros_like(q_pos)
    for d in range(1, 16):
        begin = start_ref[d : d + 1, :]
        low = jnp.where(begin <= q_pos, begin, low)
        low_first = jnp.where(begin <= group * GROUP, begin, low_first)
    low_s[...] = low
    bias_s[...] = jnp.where(low == low_first, 0.0, MASKED)
    low_group = lax.shift_right_logical(low_first, 7)
    plan[16:32, :] = group
    plan[32:48, :] = low_group
    begin_at = jnp.sum(jnp.where(lane16 <= low_group, here, 0), axis=1, keepdims=True)
    end_at = jnp.sum(jnp.where(lane16 < group, here, 0), axis=1, keepdims=True)
    tiles = lax.shift_right_logical(jnp.maximum(end_at - begin_at, 0) + (TILE - 1), 2)
    begin_at, end_at, tiles = (jnp.broadcast_to(x, (16, 128)) for x in (begin_at, end_at, tiles))
    done = jnp.zeros((1, 128), jnp.int32)
    item = [lane, lane + 128, lane + 256]
    item_u, item_at, item_end = [[jnp.zeros((1, 128), jnp.int32) for _ in item] for _ in range(3)]
    for u in range(16):
        after = done + tiles[u : u + 1, :]
        for i, n in enumerate(item):
            mine = (done <= n) & (n < after)
            item_u[i] = jnp.where(mine, u, item_u[i])
            item_at[i] = jnp.where(mine, begin_at[u : u + 1, :] + (n - done) * TILE, item_at[i])
            item_end[i] = jnp.where(mine, end_at[u : u + 1, :], item_end[i])
        done = after
    for i in range(3):
        plan[2 + i : 3 + i, :] = item_u[i]
        plan[5 + i : 6 + i, :] = item_at[i]
        plan[8 + i : 9 + i, :] = item_end[i]
    plan[11:12, :] = done
    copy = pltpu.make_async_copy(plan, sm, sem)
    copy.start()
    copy.wait()

    row = lax.broadcasted_iota(jnp.int32, (GROUP, GROUP), 0)

    def half(slot, base):
        return pl.ds(pl.multiple_of(base + lax.rem(slot, 2) * GROUP, 16), GROUP)

    def queries_of(u):
        return q[lax.rem(u, 8), pl.ds(pl.multiple_of(lax.div(u, 8) * GROUP, GROUP), GROUP), :]

    def edges(u):
        g, low_g = sm[16 + u, 0], sm[32 + u, 0]
        q_t = queries_of(u)
        lower = low_s[pl.ds(u, 1), :]
        upper = g * GROUP + lane
        scores, held = [], []
        for key_group, wanted in ((g, True), (low_g, low_g < g)):
            found = sm[1, key_group]
            slot = jnp.maximum(found, 0)
            base = jnp.where((found >= 0) & wanted, key_group * GROUP, FAR)
            one = jnp.dot(kv[lax.div(slot, 2), half(slot, 0), :], q_t, preferred_element_type=jnp.float32)
            seen = (row >= lower - base) & (row <= upper - base)
            scores.append(jnp.where(seen, one, MASKED))
            held.append(kv[lax.div(slot, 2), half(slot, K_ROWS), :])
        top = jnp.full((1, GROUP), NEG, jnp.float32)
        for one in scores:
            top = jnp.maximum(top, jnp.max(one, axis=0, keepdims=True))
        parts = [jnp.exp2((one - top) * COEF) for one in scores]
        top_s[pl.ds(u, 1), :] = top
        weight_s[pl.ds(u, 1), :] = sum(jnp.sum(part, axis=0, keepdims=True) for part in parts)
        acc_s[u] = jnp.dot(
            jnp.concatenate(held, axis=1),
            jnp.concatenate([part.astype(jnp.bfloat16) for part in parts], axis=0),
            preferred_element_type=jnp.float32,
        )

    @pl.loop(0, 4)
    def _(k):
        for n in range(4):
            edges(4 * k + n)

    def read(i):
        r, k = lax.shift_right_logical(i, 7), lax.bitwise_and(i, 127)
        return sm[2 + r, k], sm[5 + r, k], sm[8 + r, k]

    def slot_of(e, end):
        return lax.shift_right_logical(sm[0, jnp.maximum(jnp.minimum(e, end - 1), 0)], 7)

    def score(i, dst):
        u, e, end = read(i)
        q_t = queries_of(u)
        for j in range(TILE):
            slot = slot_of(e + j, end)
            dst[j * GROUP : (j + 1) * GROUP, :] = jnp.dot(
                kv[lax.div(slot, 2), half(slot, 0), :], q_t, preferred_element_type=jnp.float32
            )

    def absorb(i, src):
        u, e, end = read(i)
        lanes = bias_s[pl.ds(u, 1), :]
        top = top_s[pl.ds(u, 1), :]
        new_top, biases, held, parts = top, [], [], []
        for j in range(TILE):
            biases.append(jnp.where(e + j < end, lanes, MASKED))
            best = jnp.max(src[j * GROUP : (j + 1) * GROUP, :], axis=0, keepdims=True)
            new_top = jnp.maximum(new_top, best + biases[j])
        factor = jnp.exp2((top - new_top) * COEF)
        weight = weight_s[pl.ds(u, 1), :] * factor
        for j in range(TILE):
            part = jnp.exp2((src[j * GROUP : (j + 1) * GROUP, :] - (new_top - biases[j])) * COEF)
            weight = weight + jnp.sum(part, axis=0, keepdims=True)
            parts.append(part.astype(jnp.bfloat16))
            slot = slot_of(e + j, end)
            held.append(kv[lax.div(slot, 2), half(slot, K_ROWS), :])
        top_s[pl.ds(u, 1), :] = new_top
        weight_s[pl.ds(u, 1), :] = weight
        acc_s[u] = acc_s[u] * factor + jnp.dot(
            jnp.concatenate(held, axis=1), jnp.concatenate(parts, axis=0), preferred_element_type=jnp.float32
        )

    total = sm[11, 0]
    score(jnp.int32(0), s_even)

    @pl.loop(0, lax.shift_right_logical(total + 7, 3))
    def _(k):
        for n in range(0, 8, 2):
            i = 8 * k + n
            score(i + 1, s_odd)
            absorb(i, s_even)
            score(i + 2, s_even)
            absorb(i + 1, s_odd)

    @pl.loop(0, 16, unroll=4)
    def _(u):
        weight = weight_s[pl.ds(u, 1), :]
        some = weight > 0.0
        safe = jnp.where(some, weight, 1.0)
        ch, s = lax.rem(u, 8), lax.div(u, 8)
        o_ref[ch, pl.ds(pl.multiple_of(s * GROUP, GROUP), GROUP), :] = (acc_s[u] * (1.0 / safe)).astype(jnp.bfloat16)
        l_ref[ch, pl.ds(s, 1), :] = jnp.where(some, top_s[pl.ds(u, 1), :] * COEF + jnp.log2(safe), NEG)


def merge_kernel(o_ref, l_ref, out_ref, o_in, l_in, snd, orecv, lrecv):
    z, y, xh, c, hd = place()
    zs = [z, lax.rem(z + 1, 4), lax.rem(z + 2, 4), lax.rem(z + 3, 4)]
    peers = [(dz, dx) for dz in (2, 1, 3, 0) for dx in (1, 0) if dz or dx]
    barrier = pltpu.get_barrier_semaphore()
    for dz, dx in peers:
        to = (zs[dz], y, 1 - xh if dx else xh, c, hd)
        pl.semaphore_signal(barrier, inc=1, device_id=to, device_id_type=MESH)
    mine = z * 2 + xh
    o_in[mine] = o_ref[mine]
    l_in[mine] = l_ref[mine]
    pl.semaphore_wait(barrier, len(peers))
    sent = []
    for n, (dz, dx) in enumerate(peers):
        side = 1 - xh if dx else xh
        to, theirs = (zs[dz], y, side, c, hd), zs[dz] * 2 + side
        for src, dst, recv in ((o_ref, o_in, orecv), (l_ref, l_in, lrecv)):
            copy = remote(src.at[theirs], dst.at[mine], snd.at[len(sent)], recv.at[dz * 2 + dx], to)
            copy.start()
            sent.append(copy)
    for dz, dx in peers:
        side = 1 - xh if dx else xh
        theirs = zs[(4 - dz) % 4] * 2 + side
        to = (zs[1], y, xh, c, hd)
        remote(o_ref.at[0], o_in.at[theirs], snd.at[0], orecv.at[dz * 2 + dx], to).wait_recv()
        remote(l_ref.at[0], l_in.at[theirs], snd.at[0], lrecv.at[dz * 2 + dx], to).wait_recv()
    for h in range(4):
        for s in range(2):
            rows = slice(s * GROUP, (s + 1) * GROUP)
            a, b = l_in[2 * h, s : s + 1, :], l_in[2 * h + 1, s : s + 1, :]
            most = jnp.maximum(a, b)
            wa, wb = jnp.exp2(a - most), jnp.exp2(b - most)
            total = wa + wb
            merged = o_in[2 * h, rows, :].astype(jnp.float32) * (wa / total)
            merged = merged + o_in[2 * h + 1, rows, :].astype(jnp.float32) * (wb / total)
            out_ref[rows, h * HEAD_DIM : (h + 1) * HEAD_DIM] = merged.T.astype(jnp.bfloat16)
    for copy in sent:
        copy.wait_send()


def shards(queries, keys, values, group_table, doc_ids):
    vmem = pl.BlockSpec(memory_space=pltpu.VMEM)
    hbm = pl.BlockSpec(memory_space=pltpu.HBM)
    dma = pltpu.SemaphoreType.DMA
    kv, q, begins = pl.pallas_call(
        spread_kernel,
        out_shape=(
            pltpu.VMEM((32, CHUNK, HEAD_DIM), jnp.bfloat16),
            pltpu.VMEM((8, Q_ROWS, HEAD_DIM), jnp.bfloat16),
            pltpu.VMEM((16, 128), jnp.int32),
        ),
        in_specs=[hbm] * 5,
        out_specs=(vmem, vmem, vmem),
        scratch_shapes=[
            pltpu.VMEM((4, Q_AT + Q_ROWS, HEAD_DIM), jnp.bfloat16),
            pltpu.VMEM(queries.shape, jnp.bfloat16),
            pltpu.VMEM(values.shape, jnp.bfloat16),
            pltpu.VMEM((128, 128), jnp.int32),
            pltpu.SMEM((1, 2), jnp.int32),
            dma((8,)), dma((69,)), dma((4, 2)), dma((4, 2)), dma((4, 2)), dma((4, 2)), dma((4, 4, 2)), dma((8,)),
        ],
        compiler_params=pltpu.CompilerParams(collective_id=0, has_side_effects=True, vmem_limit_bytes=62050000),
    )(queries, keys, values, group_table, doc_ids.reshape(128, 128))
    o, l = pl.pallas_call(
        attend_kernel,
        out_shape=(
            pltpu.VMEM((8, 2 * GROUP, HEAD_DIM), jnp.bfloat16),
            pltpu.VMEM((8, 8, GROUP), jnp.float32),
        ),
        in_specs=[vmem, vmem, vmem],
        out_specs=(vmem, vmem),
        scratch_shapes=[
            pltpu.VMEM((48, 128), jnp.int32),
            pltpu.SMEM((48, 128), jnp.int32),
            pltpu.VMEM((16, 128), jnp.int32),
            pltpu.VMEM((16, 128), jnp.float32),
            pltpu.VMEM((16, 128), jnp.float32),
            pltpu.VMEM((16, 128), jnp.float32),
            pltpu.VMEM((16, HEAD_DIM, GROUP), jnp.float32),
            pltpu.VMEM((TILE * GROUP, GROUP), jnp.float32),
            pltpu.VMEM((TILE * GROUP, GROUP), jnp.float32),
            dma,
        ],
        compiler_params=pltpu.CompilerParams(vmem_limit_bytes=16 << 20),
    )(kv, q, begins)
    return pl.pallas_call(
        merge_kernel,
        out_shape=jax.ShapeDtypeStruct(queries.shape, jnp.bfloat16),
        in_specs=[vmem, vmem],
        out_specs=vmem,
        scratch_shapes=[
            pltpu.VMEM((8, 2 * GROUP, HEAD_DIM), jnp.bfloat16),
            pltpu.VMEM((8, 8, GROUP), jnp.float32),
            dma((14,)), dma((8,)), dma((8,)),
        ],
        compiler_params=pltpu.CompilerParams(collective_id=1, has_side_effects=True, vmem_limit_bytes=16 << 20),
    )(o, l)


def solution(mesh):
    split = Mesh(mesh.devices.reshape(4, 4, 2, 2, mesh.shape["head"]), AXES)
    return jax.shard_map(
        shards,
        mesh=split,
        in_specs=(P(BLK, "head"), P(BLK, "head"), P(BLK, "head"), P(BLK, None), P()),
        out_specs=P(BLK, "head"),
        check_vma=False,
    )
```

```python
import math

import jax
import jax.numpy as jnp
from jax import lax
from jax.experimental import pallas as pl
from jax.experimental.pallas import tpu as pltpu
from jax.sharding import Mesh
from jax.sharding import PartitionSpec as P

HEAD_DIM = 128
GROUP = 128
GROUPS = 128
AXES = ("z", "y", "xh", "core", "head")
BLK = AXES[:4]
MESH = pl.DeviceIdType.MESH
K_ROWS = 2 * GROUP + 16
CHUNK = K_ROWS + 2 * GROUP
Q_AT, Q_ROWS = CHUNK, 2 * GROUP + 16
NEG = -1e30
MASKED = -3e38
FAR = 1 << 20
TILE = 4
COEF = math.log2(math.e) / math.sqrt(HEAD_DIM)


def place():
    return tuple(lax.axis_index(a) for a in AXES)


def remote(src, dst, send, recv, to):
    return pltpu.make_async_remote_copy(
        src_ref=src, dst_ref=dst, send_sem=send, recv_sem=recv, device_id=to, device_id_type=MESH
    )


def spread_kernel(
    q_hbm, k_hbm, v_hbm, table_hbm, doc_hbm, kv_out, q_out, start_out, src, q_in, v_in, docs, table, loc, snd, own, yp, ym, rl, dd, qr
):
    z, y, xh, c, hd = place()
    up, down, over = lax.rem(y + 1, 4), lax.rem(y + 3, 4), lax.rem(y + 2, 4)
    zs = [z, lax.rem(z + 1, 4), lax.rem(z + 2, 4), lax.rem(z + 3, 4)]
    to_up, to_down, to_core = (z, up, xh, c, hd), (z, down, xh, c, hd), (z, y, xh, 1 - c, hd)
    local = [
        pltpu.make_async_copy(table_hbm, table, loc.at[0]),
        pltpu.make_async_copy(v_hbm, v_in, loc.at[1]),
        pltpu.make_async_copy(q_hbm, q_in, loc.at[2]),
        pltpu.make_async_copy(doc_hbm, docs, loc.at[3]),
    ]
    for h in range(4):
        keys_of_head = k_hbm.at[:, pl.ds(h * HEAD_DIM, HEAD_DIM)]
        local.append(pltpu.make_async_copy(keys_of_head, src.at[h, pl.ds(0, 2 * GROUP)], loc.at[4 + h]))
    for copy in local:
        copy.start()
    partners = [(zs[dz], y, xh, c, hd) for dz in (1, 2, 3)]
    partners += [(zs[dz], y, 1 - xh, c, hd) for dz in range(4)] + [to_up, to_down, to_core]
    barrier = pltpu.get_barrier_semaphore()
    for to in partners:
        pl.semaphore_signal(barrier, inc=1, device_id=to, device_id_type=MESH)

    local[0].wait()
    first = table[0, 0].astype(jnp.float32)
    for h in range(4):
        header = jnp.full((16, HEAD_DIM), first, jnp.float32).astype(jnp.bfloat16)
        src[h, K_ROWS - 16 : K_ROWS, :] = header
        src[h, Q_AT + 2 * GROUP :, :] = header
    local[1].wait()
    for h in range(4):
        for s in range(2):
            rows, cols = slice(s * GROUP, (s + 1) * GROUP), slice(h * HEAD_DIM, (h + 1) * HEAD_DIM)
            src[h, K_ROWS + s * GROUP : K_ROWS + (s + 1) * GROUP, :] = v_in[rows, cols].T
    for copy in local[2:]:
        copy.wait()
    pl.semaphore_wait(barrier, len(partners))

    sent = []

    def start(src_ref, dst_ref, recv, to):
        copy = remote(src_ref, dst_ref, snd.at[len(sent)], recv, to)
        copy.start()
        sent.append(copy)

    def landed(dst_ref, recv):
        remote(dst_ref, dst_ref, snd.at[0], recv, to_core).wait_recv()

    span = (pl.ds(0, K_ROWS), pl.ds(K_ROWS, 2 * GROUP))

    def piece(zz, yy, cc, p):
        return kv_out.at[(zz * 4 + yy) * 2 + cc, span[p]]

    order = (0, 1, 3, 2)
    came = [zs[(4 - dz) % 4] for dz in order]

    def first_hop(s, p):
        mine = piece(came[s], y, c, p)
        here = src.at[z, span[p]]
        if s > 0:
            landed(mine, own.at[s, p])
            here = mine
        start(here, mine, yp.at[s, p], to_up)
        start(here, mine, ym.at[s, p], to_down)
        start(here, mine, dd.at[s, 0, p], to_core)

    def second_hop(s, p):
        below, above = piece(came[s], down, c, p), piece(came[s], up, c, p)
        ways = [(below, yp, to_up, 1), (above, ym, to_down, 2)]
        for ref, came_in, onward, i in ways if p == 0 else ways[::-1]:
            landed(ref, came_in.at[s, p])
            if i == 1 + p:
                start(ref, ref, rl.at[s, p], onward)
            start(ref, ref, dd.at[s, i, p], to_core)

    def last_hop(s, p):
        across = piece(came[s], over, c, p)
        landed(across, rl.at[s, p])
        start(across, across, dd.at[s, 3, p], to_core)

    first_hop(0, 0)
    for s, p in ((1, 0), (2, 0), (1, 1), (2, 1), (3, 0), (3, 1)):
        dz = order[s]
        start(src.at[zs[dz], span[p]], piece(z, y, c, p), own.at[s, p], (zs[dz], y, xh, c, hd))
    first_hop(0, 1)
    kv_out[(z * 4 + y) * 2 + c] = src[z, 0:CHUNK]
    for h in range(4):
        for s in range(2):
            rows, cols = slice(s * GROUP, (s + 1) * GROUP), slice(h * HEAD_DIM, (h + 1) * HEAD_DIM)
            src[h, Q_AT + s * GROUP : Q_AT + (s + 1) * GROUP, :] = q_in[rows, cols].T
    held = docs[...]
    for d in range(16):
        counted = jnp.sum(jnp.where(held < d, 1, 0), axis=0, keepdims=True)
        start_out[d : d + 1, :] = jnp.broadcast_to(jnp.sum(counted, axis=1, keepdims=True), (1, 128))
    q_span, q_mine = pl.ds(Q_AT, Q_ROWS), q_out.at[z * 2 + xh]
    q_out[z * 2 + xh] = src[z, Q_AT:]
    def send_queries():
        for dz in (1, 3, 2, 0):
            for dx in (1, 0):
                if dz or dx:
                    start(src.at[zs[dz], q_span], q_mine, qr.at[dz * 2 + dx], (zs[dz], y, 1 - xh if dx else xh, c, hd))

    for s in range(1, 4):
        for p in range(2):
            first_hop(s, p)
            second_hop(s - 1, p)
            if s > 1:
                last_hop(s - 2, p)
        if s == 2:
            send_queries()
    for p in range(2):
        second_hop(3, p)
        last_hop(2, p)
    for p in range(2):
        last_hop(3, p)

    for dz in range(4):
        for dx in range(2):
            if dz or dx:
                landed(q_out.at[zs[(4 - dz) % 4] * 2 + (1 - xh if dx else xh)], qr.at[dz * 2 + dx])
    for s in range(4):
        for i, yy in enumerate((y, down, up, over)):
            for p in range(2):
                landed(piece(came[s], yy, 1 - c, p), dd.at[s, i, p])
    for copy in sent:
        copy.wait_send()


def attend_kernel(kv, q, start_ref, o_ref, l_ref, plan, sm, low_s, bias_s, top_s, weight_s, acc_s, s_even, s_odd, sem):
    lane = lax.broadcasted_iota(jnp.int32, (1, 128), 1)
    lane32 = lax.broadcasted_iota(jnp.int32, (32, 128), 1)
    lane16 = lax.broadcasted_iota(jnp.int32, (16, 128), 1)
    code = lax.broadcasted_iota(jnp.int32, (32, 128), 0) * 2
    first = kv[:, 2 * GROUP, :].astype(jnp.float32).astype(jnp.int32)
    second = GROUPS - 1 - first
    at = jnp.where(first == lane32, code + 1, 0) + jnp.where(second == lane32, code + 2, 0)
    inv = jnp.sum(at, axis=0, keepdims=True) - 1
    here = jnp.where(inv >= 0, 1, 0)
    rank0 = jnp.sum(jnp.where(lane32 < first, here, 0), axis=1, keepdims=True)
    rank1 = jnp.sum(jnp.where(lane32 < second, here, 0), axis=1, keepdims=True)
    listed = jnp.where(rank0 == lane32, code * GROUPS, 0) + jnp.where(rank1 == lane32, (code + 1) * GROUPS, 0)
    plan[0:1, :] = jnp.sum(listed, axis=0, keepdims=True)
    plan[1:2, :] = inv

    q_first = q[:, 2 * GROUP, :].astype(jnp.float32).astype(jnp.int32)
    group = jnp.concatenate([q_first, GROUPS - 1 - q_first], axis=0)
    q_pos = group * GROUP + lane16
    low, low_first = jnp.zeros_like(q_pos), jnp.zeros_like(q_pos)
    for d in range(1, 16):
        begin = start_ref[d : d + 1, :]
        low = jnp.where(begin <= q_pos, begin, low)
        low_first = jnp.where(begin <= group * GROUP, begin, low_first)
    low_s[...] = low
    bias_s[...] = jnp.where(low == low_first, 0.0, MASKED)
    low_group = lax.shift_right_logical(low_first, 7)
    plan[16:32, :] = group
    plan[32:48, :] = low_group
    begin_at = jnp.sum(jnp.where(lane16 <= low_group, here, 0), axis=1, keepdims=True)
    end_at = jnp.sum(jnp.where(lane16 < group, here, 0), axis=1, keepdims=True)
    tiles = lax.shift_right_logical(jnp.maximum(end_at - begin_at, 0) + (TILE - 1), 2)
    begin_at, end_at, tiles = (jnp.broadcast_to(x, (16, 128)) for x in (begin_at, end_at, tiles))
    done = jnp.zeros((1, 128), jnp.int32)
    item = [lane, lane + 128, lane + 256]
    item_u, item_at, item_end = [[jnp.zeros((1, 128), jnp.int32) for _ in item] for _ in range(3)]
    for u in range(16):
        after = done + tiles[u : u + 1, :]
        for i, n in enumerate(item):
            mine = (done <= n) & (n < after)
            item_u[i] = jnp.where(mine, u, item_u[i])
            item_at[i] = jnp.where(mine, begin_at[u : u + 1, :] + (n - done) * TILE, item_at[i])
            item_end[i] = jnp.where(mine, end_at[u : u + 1, :], item_end[i])
        done = after
    for i in range(3):
        plan[2 + i : 3 + i, :] = item_u[i]
        plan[5 + i : 6 + i, :] = item_at[i]
        plan[8 + i : 9 + i, :] = item_end[i]
    plan[11:12, :] = done
    copy = pltpu.make_async_copy(plan, sm, sem)
    copy.start()
    copy.wait()

    row = lax.broadcasted_iota(jnp.int32, (GROUP, GROUP), 0)

    def half(slot, base):
        return pl.ds(pl.multiple_of(base + lax.rem(slot, 2) * GROUP, 16), GROUP)

    def queries_of(u):
        return q[lax.rem(u, 8), pl.ds(pl.multiple_of(lax.div(u, 8) * GROUP, GROUP), GROUP), :]

    def edges(u):
        g, low_g = sm[16 + u, 0], sm[32 + u, 0]
        q_t = queries_of(u)
        lower = low_s[pl.ds(u, 1), :]
        upper = g * GROUP + lane
        scores, held = [], []
        for key_group, wanted in ((g, True), (low_g, low_g < g)):
            found = sm[1, key_group]
            slot = jnp.maximum(found, 0)
            base = jnp.where((found >= 0) & wanted, key_group * GROUP, FAR)
            one = jnp.dot(kv[lax.div(slot, 2), half(slot, 0), :], q_t, preferred_element_type=jnp.float32)
            seen = (row >= lower - base) & (row <= upper - base)
            scores.append(jnp.where(seen, one, MASKED))
            held.append(kv[lax.div(slot, 2), half(slot, K_ROWS), :])
        top = jnp.full((1, GROUP), NEG, jnp.float32)
        for one in scores:
            top = jnp.maximum(top, jnp.max(one, axis=0, keepdims=True))
        parts = [jnp.exp2((one - top) * COEF) for one in scores]
        top_s[pl.ds(u, 1), :] = top
        weight_s[pl.ds(u, 1), :] = sum(jnp.sum(part, axis=0, keepdims=True) for part in parts)
        acc_s[u] = jnp.dot(
            jnp.concatenate(held, axis=1),
            jnp.concatenate([part.astype(jnp.bfloat16) for part in parts], axis=0),
            preferred_element_type=jnp.float32,
        )

    @pl.loop(0, 2)
    def _(k):
        for n in range(8):
            edges(8 * k + n)

    def read(i):
        r, k = lax.shift_right_logical(i, 7), lax.bitwise_and(i, 127)
        return sm[2 + r, k], sm[5 + r, k], sm[8 + r, k]

    def slot_of(e, end):
        return lax.shift_right_logical(sm[0, jnp.maximum(jnp.minimum(e, end - 1), 0)], 7)

    def score(i, dst):
        u, e, end = read(i)
        q_t = queries_of(u)
        for j in range(TILE):
            slot = slot_of(e + j, end)
            dst[j * GROUP : (j + 1) * GROUP, :] = jnp.dot(
                kv[lax.div(slot, 2), half(slot, 0), :], q_t, preferred_element_type=jnp.float32
            )

    def absorb(i, src):
        u, e, end = read(i)
        lanes = bias_s[pl.ds(u, 1), :]
        top = top_s[pl.ds(u, 1), :]
        new_top, biases, held, parts = top, [], [], []
        for j in range(TILE):
            biases.append(jnp.where(e + j < end, lanes, MASKED))
            best = jnp.max(src[j * GROUP : (j + 1) * GROUP, :], axis=0, keepdims=True)
            new_top = jnp.maximum(new_top, best + biases[j])
        factor = jnp.exp2((top - new_top) * COEF)
        weight = weight_s[pl.ds(u, 1), :] * factor
        for j in range(TILE):
            part = jnp.exp2((src[j * GROUP : (j + 1) * GROUP, :] - (new_top - biases[j])) * COEF)
            weight = weight + jnp.sum(part, axis=0, keepdims=True)
            parts.append(part.astype(jnp.bfloat16))
            slot = slot_of(e + j, end)
            held.append(kv[lax.div(slot, 2), half(slot, K_ROWS), :])
        top_s[pl.ds(u, 1), :] = new_top
        weight_s[pl.ds(u, 1), :] = weight
        acc_s[u] = acc_s[u] * factor + jnp.dot(
            jnp.concatenate(held, axis=1), jnp.concatenate(parts, axis=0), preferred_element_type=jnp.float32
        )

    total = sm[11, 0]
    score(jnp.int32(0), s_even)

    @pl.loop(0, lax.shift_right_logical(total + 7, 3))
    def _(k):
        for n in range(0, 8, 2):
            i = 8 * k + n
            score(i + 1, s_odd)
            absorb(i, s_even)
            score(i + 2, s_even)
            absorb(i + 1, s_odd)

    @pl.loop(0, 16, unroll=4)
    def _(u):
        weight = weight_s[pl.ds(u, 1), :]
        some = weight > 0.0
        safe = jnp.where(some, weight, 1.0)
        ch, s = lax.rem(u, 8), lax.div(u, 8)
        o_ref[ch, pl.ds(pl.multiple_of(s * GROUP, GROUP), GROUP), :] = (acc_s[u] * (1.0 / safe)).astype(jnp.bfloat16)
        l_ref[ch, pl.ds(s, 1), :] = jnp.where(some, top_s[pl.ds(u, 1), :] * COEF + jnp.log2(safe), NEG)


def merge_kernel(o_ref, l_ref, out_ref, o_in, l_in, snd, orecv, lrecv):
    z, y, xh, c, hd = place()
    zs = [z, lax.rem(z + 1, 4), lax.rem(z + 2, 4), lax.rem(z + 3, 4)]
    peers = [(dz, dx) for dz in (2, 1, 3, 0) for dx in (1, 0) if dz or dx]
    barrier = pltpu.get_barrier_semaphore()
    for dz, dx in peers:
        to = (zs[dz], y, 1 - xh if dx else xh, c, hd)
        pl.semaphore_signal(barrier, inc=1, device_id=to, device_id_type=MESH)
    mine = z * 2 + xh
    o_in[mine] = o_ref[mine]
    l_in[mine] = l_ref[mine]
    pl.semaphore_wait(barrier, len(peers))
    sent = []
    for n, (dz, dx) in enumerate(peers):
        side = 1 - xh if dx else xh
        to, theirs = (zs[dz], y, side, c, hd), zs[dz] * 2 + side
        for src, dst, recv in ((o_ref, o_in, orecv), (l_ref, l_in, lrecv)):
            copy = remote(src.at[theirs], dst.at[mine], snd.at[len(sent)], recv.at[dz * 2 + dx], to)
            copy.start()
            sent.append(copy)
    for dz, dx in peers:
        side = 1 - xh if dx else xh
        theirs = zs[(4 - dz) % 4] * 2 + side
        to = (zs[1], y, xh, c, hd)
        remote(o_ref.at[0], o_in.at[theirs], snd.at[0], orecv.at[dz * 2 + dx], to).wait_recv()
        remote(l_ref.at[0], l_in.at[theirs], snd.at[0], lrecv.at[dz * 2 + dx], to).wait_recv()
    for h in range(4):
        for s in range(2):
            rows = slice(s * GROUP, (s + 1) * GROUP)
            a, b = l_in[2 * h, s : s + 1, :], l_in[2 * h + 1, s : s + 1, :]
            most = jnp.maximum(a, b)
            wa, wb = jnp.exp2(a - most), jnp.exp2(b - most)
            total = wa + wb
            merged = o_in[2 * h, rows, :].astype(jnp.float32) * (wa / total)
            merged = merged + o_in[2 * h + 1, rows, :].astype(jnp.float32) * (wb / total)
            out_ref[rows, h * HEAD_DIM : (h + 1) * HEAD_DIM] = merged.T.astype(jnp.bfloat16)
    for copy in sent:
        copy.wait_send()


def shards(queries, keys, values, group_table, doc_ids):
    vmem = pl.BlockSpec(memory_space=pltpu.VMEM)
    hbm = pl.BlockSpec(memory_space=pltpu.HBM)
    dma = pltpu.SemaphoreType.DMA
    kv, q, begins = pl.pallas_call(
        spread_kernel,
        out_shape=(
            pltpu.VMEM((32, CHUNK, HEAD_DIM), jnp.bfloat16),
            pltpu.VMEM((8, Q_ROWS, HEAD_DIM), jnp.bfloat16),
            pltpu.VMEM((16, 128), jnp.int32),
        ),
        in_specs=[hbm] * 5,
        out_specs=(vmem, vmem, vmem),
        scratch_shapes=[
            pltpu.VMEM((4, Q_AT + Q_ROWS, HEAD_DIM), jnp.bfloat16),
            pltpu.VMEM(queries.shape, jnp.bfloat16),
            pltpu.VMEM(values.shape, jnp.bfloat16),
            pltpu.VMEM((128, 128), jnp.int32),
            pltpu.SMEM((1, 2), jnp.int32),
            dma((8,)), dma((69,)), dma((4, 2)), dma((4, 2)), dma((4, 2)), dma((4, 2)), dma((4, 4, 2)), dma((8,)),
        ],
        compiler_params=pltpu.CompilerParams(collective_id=0, has_side_effects=True, vmem_limit_bytes=62050000),
    )(queries, keys, values, group_table, doc_ids.reshape(128, 128))
    o, l = pl.pallas_call(
        attend_kernel,
        out_shape=(
            pltpu.VMEM((8, 2 * GROUP, HEAD_DIM), jnp.bfloat16),
            pltpu.VMEM((8, 8, GROUP), jnp.float32),
        ),
        in_specs=[vmem, vmem, vmem],
        out_specs=(vmem, vmem),
        scratch_shapes=[
            pltpu.VMEM((48, 128), jnp.int32),
            pltpu.SMEM((48, 128), jnp.int32),
            pltpu.VMEM((16, 128), jnp.int32),
            pltpu.VMEM((16, 128), jnp.float32),
            pltpu.VMEM((16, 128), jnp.float32),
            pltpu.VMEM((16, 128), jnp.float32),
            pltpu.VMEM((16, HEAD_DIM, GROUP), jnp.float32),
            pltpu.VMEM((TILE * GROUP, GROUP), jnp.float32),
            pltpu.VMEM((TILE * GROUP, GROUP), jnp.float32),
            dma,
        ],
        compiler_params=pltpu.CompilerParams(vmem_limit_bytes=16 << 20),
    )(kv, q, begins)
    return pl.pallas_call(
        merge_kernel,
        out_shape=jax.ShapeDtypeStruct(queries.shape, jnp.bfloat16),
        in_specs=[vmem, vmem],
        out_specs=vmem,
        scratch_shapes=[
            pltpu.VMEM((8, 2 * GROUP, HEAD_DIM), jnp.bfloat16),
            pltpu.VMEM((8, 8, GROUP), jnp.float32),
            dma((14,)), dma((8,)), dma((8,)),
        ],
        compiler_params=pltpu.CompilerParams(collective_id=1, has_side_effects=True, vmem_limit_bytes=16 << 20),
    )(o, l)


def solution(mesh):
    split = Mesh(mesh.devices.reshape(4, 4, 2, 2, mesh.shape["head"]), AXES)
    return jax.shard_map(
        shards,
        mesh=split,
        in_specs=(P(BLK, "head"), P(BLK, "head"), P(BLK, "head"), P(BLK, None), P()),
        out_specs=P(BLK, "head"),
        check_vma=False,
    )
```

```python
import math

import jax
import jax.numpy as jnp
from jax import lax
from jax.experimental import pallas as pl
from jax.experimental.pallas import tpu as pltpu
from jax.sharding import Mesh
from jax.sharding import PartitionSpec as P

HEAD_DIM = 128
GROUP = 128
GROUPS = 128
AXES = ("z", "y", "xh", "core", "head")
BLK = AXES[:4]
MESH = pl.DeviceIdType.MESH
K_ROWS = 2 * GROUP + 16
CHUNK = K_ROWS + 2 * GROUP
Q_AT, Q_ROWS = CHUNK, 2 * GROUP + 16
NEG = -1e30
MASKED = -3e38
FAR = 1 << 20
TILE = 4
COEF = math.log2(math.e) / math.sqrt(HEAD_DIM)


def place():
    return tuple(lax.axis_index(a) for a in AXES)


def remote(src, dst, send, recv, to):
    return pltpu.make_async_remote_copy(
        src_ref=src, dst_ref=dst, send_sem=send, recv_sem=recv, device_id=to, device_id_type=MESH
    )


def spread_kernel(
    q_hbm, k_hbm, v_hbm, table_hbm, doc_hbm, kv_out, q_out, start_out, src, q_in, v_in, docs, table, loc, snd, own, yp, ym, rl, dd, qr
):
    z, y, xh, c, hd = place()
    up, down, over = lax.rem(y + 1, 4), lax.rem(y + 3, 4), lax.rem(y + 2, 4)
    zs = [z, lax.rem(z + 1, 4), lax.rem(z + 2, 4), lax.rem(z + 3, 4)]
    to_up, to_down, to_core = (z, up, xh, c, hd), (z, down, xh, c, hd), (z, y, xh, 1 - c, hd)
    local = [
        pltpu.make_async_copy(table_hbm, table, loc.at[0]),
        pltpu.make_async_copy(v_hbm, v_in, loc.at[1]),
        pltpu.make_async_copy(q_hbm, q_in, loc.at[2]),
        pltpu.make_async_copy(doc_hbm, docs, loc.at[3]),
    ]
    for h in range(4):
        keys_of_head = k_hbm.at[:, pl.ds(h * HEAD_DIM, HEAD_DIM)]
        local.append(pltpu.make_async_copy(keys_of_head, src.at[h, pl.ds(0, 2 * GROUP)], loc.at[4 + h]))
    for copy in local:
        copy.start()
    partners = [(zs[dz], y, xh, c, hd) for dz in (1, 2, 3)]
    partners += [(zs[dz], y, 1 - xh, c, hd) for dz in range(4)] + [to_up, to_down, to_core]
    barrier = pltpu.get_barrier_semaphore()
    for to in partners:
        pl.semaphore_signal(barrier, inc=1, device_id=to, device_id_type=MESH)

    local[0].wait()
    first = table[0, 0].astype(jnp.float32)
    for h in range(4):
        header = jnp.full((16, HEAD_DIM), first, jnp.float32).astype(jnp.bfloat16)
        src[h, K_ROWS - 16 : K_ROWS, :] = header
        src[h, Q_AT + 2 * GROUP :, :] = header
    local[1].wait()
    for h in range(4):
        for s in range(2):
            rows, cols = slice(s * GROUP, (s + 1) * GROUP), slice(h * HEAD_DIM, (h + 1) * HEAD_DIM)
            src[h, K_ROWS + s * GROUP : K_ROWS + (s + 1) * GROUP, :] = v_in[rows, cols].T
    for copy in local[2:]:
        copy.wait()
    pl.semaphore_wait(barrier, len(partners))

    sent = []

    def start(src_ref, dst_ref, recv, to):
        copy = remote(src_ref, dst_ref, snd.at[len(sent)], recv, to)
        copy.start()
        sent.append(copy)

    def landed(dst_ref, recv):
        remote(dst_ref, dst_ref, snd.at[0], recv, to_core).wait_recv()

    span = (pl.ds(0, K_ROWS), pl.ds(K_ROWS, 2 * GROUP))

    def piece(zz, yy, cc, p):
        return kv_out.at[(zz * 4 + yy) * 2 + cc, span[p]]

    order = (0, 1, 3, 2)
    came = [zs[(4 - dz) % 4] for dz in order]

    def first_hop(s, p):
        mine = piece(came[s], y, c, p)
        here = src.at[z, span[p]]
        if s > 0:
            landed(mine, own.at[s, p])
            here = mine
        start(here, mine, yp.at[s, p], to_up)
        start(here, mine, ym.at[s, p], to_down)
        start(here, mine, dd.at[s, 0, p], to_core)

    def second_hop(s, p):
        below, above = piece(came[s], down, c, p), piece(came[s], up, c, p)
        ways = [(below, yp, to_up, 1), (above, ym, to_down, 2)]
        for ref, came_in, onward, i in ways if p == 0 else ways[::-1]:
            landed(ref, came_in.at[s, p])
            if i == 1 + p:
                start(ref, ref, rl.at[s, p], onward)
            start(ref, ref, dd.at[s, i, p], to_core)

    def last_hop(s, p):
        across = piece(came[s], over, c, p)
        landed(across, rl.at[s, p])
        start(across, across, dd.at[s, 3, p], to_core)

    first_hop(0, 0)
    for s, p in ((1, 0), (2, 0), (1, 1), (2, 1), (3, 0), (3, 1)):
        dz = order[s]
        start(src.at[zs[dz], span[p]], piece(z, y, c, p), own.at[s, p], (zs[dz], y, xh, c, hd))
    first_hop(0, 1)
    kv_out[(z * 4 + y) * 2 + c] = src[z, 0:CHUNK]
    for h in range(4):
        for s in range(2):
            rows, cols = slice(s * GROUP, (s + 1) * GROUP), slice(h * HEAD_DIM, (h + 1) * HEAD_DIM)
            src[h, Q_AT + s * GROUP : Q_AT + (s + 1) * GROUP, :] = q_in[rows, cols].T
    held = docs[...]
    for d in range(16):
        counted = jnp.sum(jnp.where(held < d, 1, 0), axis=0, keepdims=True)
        start_out[d : d + 1, :] = jnp.broadcast_to(jnp.sum(counted, axis=1, keepdims=True), (1, 128))
    q_span, q_mine = pl.ds(Q_AT, Q_ROWS), q_out.at[z * 2 + xh]
    q_out[z * 2 + xh] = src[z, Q_AT:]
    def send_queries():
        for dz in (1, 3, 2, 0):
            for dx in (1, 0):
                if dz or dx:
                    start(src.at[zs[dz], q_span], q_mine, qr.at[dz * 2 + dx], (zs[dz], y, 1 - xh if dx else xh, c, hd))

    for s in range(1, 4):
        for p in range(2):
            first_hop(s, p)
            second_hop(s - 1, p)
            if s > 1:
                last_hop(s - 2, p)
        if s == 2:
            send_queries()
    for p in range(2):
        second_hop(3, p)
        last_hop(2, p)
    for p in range(2):
        last_hop(3, p)

    for dz in range(4):
        for dx in range(2):
            if dz or dx:
                landed(q_out.at[zs[(4 - dz) % 4] * 2 + (1 - xh if dx else xh)], qr.at[dz * 2 + dx])
    for s in range(4):
        for i, yy in enumerate((y, down, up, over)):
            for p in range(2):
                landed(piece(came[s], yy, 1 - c, p), dd.at[s, i, p])
    for copy in sent:
        copy.wait_send()


def attend_kernel(kv, q, start_ref, o_ref, l_ref, plan, sm, low_s, bias_s, top_s, weight_s, acc_s, s_even, s_odd, sem):
    lane = lax.broadcasted_iota(jnp.int32, (1, 128), 1)
    lane32 = lax.broadcasted_iota(jnp.int32, (32, 128), 1)
    lane16 = lax.broadcasted_iota(jnp.int32, (16, 128), 1)
    code = lax.broadcasted_iota(jnp.int32, (32, 128), 0) * 2
    first = kv[:, 2 * GROUP, :].astype(jnp.float32).astype(jnp.int32)
    second = GROUPS - 1 - first
    at = jnp.where(first == lane32, code + 1, 0) + jnp.where(second == lane32, code + 2, 0)
    inv = jnp.sum(at, axis=0, keepdims=True) - 1
    here = jnp.where(inv >= 0, 1, 0)
    rank0 = jnp.sum(jnp.where(lane32 < first, here, 0), axis=1, keepdims=True)
    rank1 = jnp.sum(jnp.where(lane32 < second, here, 0), axis=1, keepdims=True)
    listed = jnp.where(rank0 == lane32, code * GROUPS, 0) + jnp.where(rank1 == lane32, (code + 1) * GROUPS, 0)
    plan[0:1, :] = jnp.sum(listed, axis=0, keepdims=True)
    plan[1:2, :] = inv

    q_first = q[:, 2 * GROUP, :].astype(jnp.float32).astype(jnp.int32)
    group = jnp.concatenate([q_first, GROUPS - 1 - q_first], axis=0)
    q_pos = group * GROUP + lane16
    low, low_first = jnp.zeros_like(q_pos), jnp.zeros_like(q_pos)
    for d in range(1, 16):
        begin = start_ref[d : d + 1, :]
        low = jnp.where(begin <= q_pos, begin, low)
        low_first = jnp.where(begin <= group * GROUP, begin, low_first)
    low_s[...] = low
    bias_s[...] = jnp.where(low == low_first, 0.0, MASKED)
    low_group = lax.shift_right_logical(low_first, 7)
    plan[16:32, :] = group
    plan[32:48, :] = low_group
    begin_at = jnp.sum(jnp.where(lane16 <= low_group, here, 0), axis=1, keepdims=True)
    end_at = jnp.sum(jnp.where(lane16 < group, here, 0), axis=1, keepdims=True)
    tiles = lax.shift_right_logical(jnp.maximum(end_at - begin_at, 0) + (TILE - 1), 2)
    begin_at, end_at, tiles = (jnp.broadcast_to(x, (16, 128)) for x in (begin_at, end_at, tiles))
    done = jnp.zeros((1, 128), jnp.int32)
    item = [lane, lane + 128, lane + 256]
    item_u, item_at, item_end = [[jnp.zeros((1, 128), jnp.int32) for _ in item] for _ in range(3)]
    for u in range(16):
        after = done + tiles[u : u + 1, :]
        for i, n in enumerate(item):
            mine = (done <= n) & (n < after)
            item_u[i] = jnp.where(mine, u, item_u[i])
            item_at[i] = jnp.where(mine, begin_at[u : u + 1, :] + (n - done) * TILE, item_at[i])
            item_end[i] = jnp.where(mine, end_at[u : u + 1, :], item_end[i])
        done = after
    for i in range(3):
        plan[2 + i : 3 + i, :] = item_u[i]
        plan[5 + i : 6 + i, :] = item_at[i]
        plan[8 + i : 9 + i, :] = item_end[i]
    plan[11:12, :] = done
    copy = pltpu.make_async_copy(plan, sm, sem)
    copy.start()
    copy.wait()

    row = lax.broadcasted_iota(jnp.int32, (GROUP, GROUP), 0)

    def half(slot, base):
        return pl.ds(pl.multiple_of(base + lax.rem(slot, 2) * GROUP, 16), GROUP)

    def queries_of(u):
        return q[lax.rem(u, 8), pl.ds(pl.multiple_of(lax.div(u, 8) * GROUP, GROUP), GROUP), :]

    def edges(u):
        g, low_g = sm[16 + u, 0], sm[32 + u, 0]
        q_t = queries_of(u)
        lower = low_s[pl.ds(u, 1), :]
        upper = g * GROUP + lane
        scores, held = [], []
        for key_group, wanted in ((g, True), (low_g, low_g < g)):
            found = sm[1, key_group]
            slot = jnp.maximum(found, 0)
            base = jnp.where((found >= 0) & wanted, key_group * GROUP, FAR)
            one = jnp.dot(kv[lax.div(slot, 2), half(slot, 0), :], q_t, preferred_element_type=jnp.float32)
            seen = (row >= lower - base) & (row <= upper - base)
            scores.append(jnp.where(seen, one, MASKED))
            held.append(kv[lax.div(slot, 2), half(slot, K_ROWS), :])
        top = jnp.full((1, GROUP), NEG, jnp.float32)
        for one in scores:
            top = jnp.maximum(top, jnp.max(one, axis=0, keepdims=True))
        parts = [jnp.exp2((one - top) * COEF) for one in scores]
        top_s[pl.ds(u, 1), :] = top
        weight_s[pl.ds(u, 1), :] = sum(jnp.sum(part, axis=0, keepdims=True) for part in parts)
        acc_s[u] = jnp.dot(
            jnp.concatenate(held, axis=1),
            jnp.concatenate([part.astype(jnp.bfloat16) for part in parts], axis=0),
            preferred_element_type=jnp.float32,
        )

    @pl.loop(0, 2)
    def _(k):
        for n in range(8):
            edges(8 * k + n)

    def read(i):
        r, k = lax.shift_right_logical(i, 7), lax.bitwise_and(i, 127)
        return sm[2 + r, k], sm[5 + r, k], sm[8 + r, k]

    def slot_of(e, end):
        return lax.shift_right_logical(sm[0, jnp.maximum(jnp.minimum(e, end - 1), 0)], 7)

    def score(i, dst):
        u, e, end = read(i)
        q_t = queries_of(u)
        for j in range(TILE):
            slot = slot_of(e + j, end)
            dst[j * GROUP : (j + 1) * GROUP, :] = jnp.dot(
                kv[lax.div(slot, 2), half(slot, 0), :], q_t, preferred_element_type=jnp.float32
            )

    def absorb(i, src):
        u, e, end = read(i)
        lanes = bias_s[pl.ds(u, 1), :]
        top = top_s[pl.ds(u, 1), :]
        new_top, biases, held, parts = top, [], [], []
        for j in range(TILE):
            biases.append(jnp.where(e + j < end, lanes, MASKED))
            best = jnp.max(src[j * GROUP : (j + 1) * GROUP, :], axis=0, keepdims=True)
            new_top = jnp.maximum(new_top, best + biases[j])
        factor = jnp.exp2((top - new_top) * COEF)
        weight = weight_s[pl.ds(u, 1), :] * factor
        for j in range(TILE):
            part = jnp.exp2((src[j * GROUP : (j + 1) * GROUP, :] - (new_top - biases[j])) * COEF)
            weight = weight + jnp.sum(part, axis=0, keepdims=True)
            parts.append(part.astype(jnp.bfloat16))
            slot = slot_of(e + j, end)
            held.append(kv[lax.div(slot, 2), half(slot, K_ROWS), :])
        top_s[pl.ds(u, 1), :] = new_top
        weight_s[pl.ds(u, 1), :] = weight
        acc_s[u] = acc_s[u] * factor + jnp.dot(
            jnp.concatenate(held, axis=1), jnp.concatenate(parts, axis=0), preferred_element_type=jnp.float32
        )

    total = sm[11, 0]
    score(jnp.int32(0), s_even)

    def run(first, count):
        for n in range(0, count, 2):
            i = first + n
            score(i + 1, s_odd)
            absorb(i, s_even)
            score(i + 2, s_even)
            absorb(i + 1, s_odd)

    eights = lax.shift_right_logical(total + 3, 3)

    @pl.loop(0, eights)
    def _(k):
        run(8 * k, 8)

    @pl.loop(0, lax.shift_right_logical(jnp.maximum(total - 8 * eights, 0) + 3, 2))
    def _(k):
        run(8 * eights + 4 * k, 4)

    @pl.loop(0, 16, unroll=4)
    def _(u):
        weight = weight_s[pl.ds(u, 1), :]
        some = weight > 0.0
        safe = jnp.where(some, weight, 1.0)
        ch, s = lax.rem(u, 8), lax.div(u, 8)
        o_ref[ch, pl.ds(pl.multiple_of(s * GROUP, GROUP), GROUP), :] = (acc_s[u] * (1.0 / safe)).astype(jnp.bfloat16)
        l_ref[ch, pl.ds(s, 1), :] = jnp.where(some, top_s[pl.ds(u, 1), :] * COEF + jnp.log2(safe), NEG)


def merge_kernel(o_ref, l_ref, out_ref, o_in, l_in, snd, orecv, lrecv):
    z, y, xh, c, hd = place()
    zs = [z, lax.rem(z + 1, 4), lax.rem(z + 2, 4), lax.rem(z + 3, 4)]
    peers = [(dz, dx) for dz in (2, 1, 3, 0) for dx in (1, 0) if dz or dx]
    barrier = pltpu.get_barrier_semaphore()
    for dz, dx in peers:
        to = (zs[dz], y, 1 - xh if dx else xh, c, hd)
        pl.semaphore_signal(barrier, inc=1, device_id=to, device_id_type=MESH)
    mine = z * 2 + xh
    o_in[mine] = o_ref[mine]
    l_in[mine] = l_ref[mine]
    pl.semaphore_wait(barrier, len(peers))
    sent = []
    for n, (dz, dx) in enumerate(peers):
        side = 1 - xh if dx else xh
        to, theirs = (zs[dz], y, side, c, hd), zs[dz] * 2 + side
        for src, dst, recv in ((o_ref, o_in, orecv), (l_ref, l_in, lrecv)):
            copy = remote(src.at[theirs], dst.at[mine], snd.at[len(sent)], recv.at[dz * 2 + dx], to)
            copy.start()
            sent.append(copy)
    for dz, dx in peers:
        side = 1 - xh if dx else xh
        theirs = zs[(4 - dz) % 4] * 2 + side
        to = (zs[1], y, xh, c, hd)
        remote(o_ref.at[0], o_in.at[theirs], snd.at[0], orecv.at[dz * 2 + dx], to).wait_recv()
        remote(l_ref.at[0], l_in.at[theirs], snd.at[0], lrecv.at[dz * 2 + dx], to).wait_recv()
    for h in range(4):
        for s in range(2):
            rows = slice(s * GROUP, (s + 1) * GROUP)
            a, b = l_in[2 * h, s : s + 1, :], l_in[2 * h + 1, s : s + 1, :]
            most = jnp.maximum(a, b)
            wa, wb = jnp.exp2(a - most), jnp.exp2(b - most)
            total = wa + wb
            merged = o_in[2 * h, rows, :].astype(jnp.float32) * (wa / total)
            merged = merged + o_in[2 * h + 1, rows, :].astype(jnp.float32) * (wb / total)
            out_ref[rows, h * HEAD_DIM : (h + 1) * HEAD_DIM] = merged.T.astype(jnp.bfloat16)
    for copy in sent:
        copy.wait_send()


def shards(queries, keys, values, group_table, doc_ids):
    vmem = pl.BlockSpec(memory_space=pltpu.VMEM)
    hbm = pl.BlockSpec(memory_space=pltpu.HBM)
    dma = pltpu.SemaphoreType.DMA
    kv, q, begins = pl.pallas_call(
        spread_kernel,
        out_shape=(
            pltpu.VMEM((32, CHUNK, HEAD_DIM), jnp.bfloat16),
            pltpu.VMEM((8, Q_ROWS, HEAD_DIM), jnp.bfloat16),
            pltpu.VMEM((16, 128), jnp.int32),
        ),
        in_specs=[hbm] * 5,
        out_specs=(vmem, vmem, vmem),
        scratch_shapes=[
            pltpu.VMEM((4, Q_AT + Q_ROWS, HEAD_DIM), jnp.bfloat16),
            pltpu.VMEM(queries.shape, jnp.bfloat16),
            pltpu.VMEM(values.shape, jnp.bfloat16),
            pltpu.VMEM((128, 128), jnp.int32),
            pltpu.SMEM((1, 2), jnp.int32),
            dma((8,)), dma((69,)), dma((4, 2)), dma((4, 2)), dma((4, 2)), dma((4, 2)), dma((4, 4, 2)), dma((8,)),
        ],
        compiler_params=pltpu.CompilerParams(collective_id=0, has_side_effects=True, vmem_limit_bytes=62050000),
    )(queries, keys, values, group_table, doc_ids.reshape(128, 128))
    o, l = pl.pallas_call(
        attend_kernel,
        out_shape=(
            pltpu.VMEM((8, 2 * GROUP, HEAD_DIM), jnp.bfloat16),
            pltpu.VMEM((8, 8, GROUP), jnp.float32),
        ),
        in_specs=[vmem, vmem, vmem],
        out_specs=(vmem, vmem),
        scratch_shapes=[
            pltpu.VMEM((48, 128), jnp.int32),
            pltpu.SMEM((48, 128), jnp.int32),
            pltpu.VMEM((16, 128), jnp.int32),
            pltpu.VMEM((16, 128), jnp.float32),
            pltpu.VMEM((16, 128), jnp.float32),
            pltpu.VMEM((16, 128), jnp.float32),
            pltpu.VMEM((16, HEAD_DIM, GROUP), jnp.float32),
            pltpu.VMEM((TILE * GROUP, GROUP), jnp.float32),
            pltpu.VMEM((TILE * GROUP, GROUP), jnp.float32),
            dma,
        ],
        compiler_params=pltpu.CompilerParams(vmem_limit_bytes=16 << 20),
    )(kv, q, begins)
    return pl.pallas_call(
        merge_kernel,
        out_shape=jax.ShapeDtypeStruct(queries.shape, jnp.bfloat16),
        in_specs=[vmem, vmem],
        out_specs=vmem,
        scratch_shapes=[
            pltpu.VMEM((8, 2 * GROUP, HEAD_DIM), jnp.bfloat16),
            pltpu.VMEM((8, 8, GROUP), jnp.float32),
            dma((14,)), dma((8,)), dma((8,)),
        ],
        compiler_params=pltpu.CompilerParams(collective_id=1, has_side_effects=True, vmem_limit_bytes=16 << 20),
    )(o, l)


def solution(mesh):
    split = Mesh(mesh.devices.reshape(4, 4, 2, 2, mesh.shape["head"]), AXES)
    return jax.shard_map(
        shards,
        mesh=split,
        in_specs=(P(BLK, "head"), P(BLK, "head"), P(BLK, "head"), P(BLK, None), P()),
        out_specs=P(BLK, "head"),
        check_vma=False,
    )
```

```python
import math

import jax
import jax.numpy as jnp
from jax import lax
from jax.experimental import pallas as pl
from jax.experimental.pallas import tpu as pltpu
from jax.sharding import Mesh
from jax.sharding import PartitionSpec as P

HEAD_DIM = 128
GROUP = 128
GROUPS = 128
AXES = ("z", "y", "xh", "core", "head")
BLK = AXES[:4]
MESH = pl.DeviceIdType.MESH
K_ROWS = 2 * GROUP + 16
CHUNK = K_ROWS + 2 * GROUP
Q_AT, Q_ROWS = CHUNK, 2 * GROUP + 16
NEG = -1e30
MASKED = -3e38
FAR = 1 << 20
TILE = 4
COEF = math.log2(math.e) / math.sqrt(HEAD_DIM)


def place():
    return tuple(lax.axis_index(a) for a in AXES)


def remote(src, dst, send, recv, to):
    return pltpu.make_async_remote_copy(
        src_ref=src, dst_ref=dst, send_sem=send, recv_sem=recv, device_id=to, device_id_type=MESH
    )


def spread_kernel(
    q_hbm, k_hbm, v_hbm, table_hbm, doc_hbm, kv_out, q_out, start_out, src, q_in, v_in, docs, table, loc, snd, own, yp, ym, rl, dd, qr
):
    z, y, xh, c, hd = place()
    up, down, over = lax.rem(y + 1, 4), lax.rem(y + 3, 4), lax.rem(y + 2, 4)
    zs = [z, lax.rem(z + 1, 4), lax.rem(z + 2, 4), lax.rem(z + 3, 4)]
    to_up, to_down, to_core = (z, up, xh, c, hd), (z, down, xh, c, hd), (z, y, xh, 1 - c, hd)
    local = [
        pltpu.make_async_copy(table_hbm, table, loc.at[0]),
        pltpu.make_async_copy(v_hbm, v_in, loc.at[1]),
        pltpu.make_async_copy(q_hbm, q_in, loc.at[2]),
        pltpu.make_async_copy(doc_hbm, docs, loc.at[3]),
    ]
    for h in range(4):
        keys_of_head = k_hbm.at[:, pl.ds(h * HEAD_DIM, HEAD_DIM)]
        local.append(pltpu.make_async_copy(keys_of_head, src.at[h, pl.ds(0, 2 * GROUP)], loc.at[4 + h]))
    for copy in local:
        copy.start()
    partners = [(zs[dz], y, xh, c, hd) for dz in (1, 2, 3)]
    partners += [(zs[dz], y, 1 - xh, c, hd) for dz in range(4)] + [to_up, to_down, to_core]
    barrier = pltpu.get_barrier_semaphore()
    for to in partners:
        pl.semaphore_signal(barrier, inc=1, device_id=to, device_id_type=MESH)

    local[0].wait()
    first = table[0, 0].astype(jnp.float32)
    for h in range(4):
        header = jnp.full((16, HEAD_DIM), first, jnp.float32).astype(jnp.bfloat16)
        src[h, K_ROWS - 16 : K_ROWS, :] = header
        src[h, Q_AT + 2 * GROUP :, :] = header
    local[1].wait()
    for h in range(4):
        for s in range(2):
            rows, cols = slice(s * GROUP, (s + 1) * GROUP), slice(h * HEAD_DIM, (h + 1) * HEAD_DIM)
            src[h, K_ROWS + s * GROUP : K_ROWS + (s + 1) * GROUP, :] = v_in[rows, cols].T
    for copy in local[2:]:
        copy.wait()
    pl.semaphore_wait(barrier, len(partners))

    sent = []

    def start(src_ref, dst_ref, recv, to):
        copy = remote(src_ref, dst_ref, snd.at[len(sent)], recv, to)
        copy.start()
        sent.append(copy)

    def landed(dst_ref, recv):
        remote(dst_ref, dst_ref, snd.at[0], recv, to_core).wait_recv()

    span = (pl.ds(0, K_ROWS), pl.ds(K_ROWS, 2 * GROUP))

    def piece(zz, yy, cc, p):
        return kv_out.at[(zz * 4 + yy) * 2 + cc, span[p]]

    order = (0, 1, 3, 2)
    came = [zs[(4 - dz) % 4] for dz in order]

    def first_hop(s, p):
        mine = piece(came[s], y, c, p)
        here = src.at[z, span[p]]
        if s > 0:
            landed(mine, own.at[s, p])
            here = mine
        start(here, mine, yp.at[s, p], to_up)
        start(here, mine, ym.at[s, p], to_down)
        start(here, mine, dd.at[s, 0, p], to_core)

    def second_hop(s, p):
        below, above = piece(came[s], down, c, p), piece(came[s], up, c, p)
        ways = [(below, yp, to_up, 1), (above, ym, to_down, 2)]
        for ref, came_in, onward, i in ways if p == 0 else ways[::-1]:
            landed(ref, came_in.at[s, p])
            if i == 1 + p:
                start(ref, ref, rl.at[s, p], onward)
            start(ref, ref, dd.at[s, i, p], to_core)

    def last_hop(s, p):
        across = piece(came[s], over, c, p)
        landed(across, rl.at[s, p])
        start(across, across, dd.at[s, 3, p], to_core)

    first_hop(0, 0)
    for s, p in ((1, 0), (2, 0), (1, 1), (2, 1), (3, 0), (3, 1)):
        dz = order[s]
        start(src.at[zs[dz], span[p]], piece(z, y, c, p), own.at[s, p], (zs[dz], y, xh, c, hd))
    first_hop(0, 1)
    kv_out[(z * 4 + y) * 2 + c] = src[z, 0:CHUNK]
    for h in range(4):
        for s in range(2):
            rows, cols = slice(s * GROUP, (s + 1) * GROUP), slice(h * HEAD_DIM, (h + 1) * HEAD_DIM)
            src[h, Q_AT + s * GROUP : Q_AT + (s + 1) * GROUP, :] = q_in[rows, cols].T
    held = docs[...]
    for d in range(16):
        counted = jnp.sum(jnp.where(held < d, 1, 0), axis=0, keepdims=True)
        start_out[d : d + 1, :] = jnp.broadcast_to(jnp.sum(counted, axis=1, keepdims=True), (1, 128))
    q_span, q_mine = pl.ds(Q_AT, Q_ROWS), q_out.at[z * 2 + xh]
    q_out[z * 2 + xh] = src[z, Q_AT:]
    def send_queries():
        for dz in (1, 3, 2, 0):
            for dx in (1, 0):
                if dz or dx:
                    start(src.at[zs[dz], q_span], q_mine, qr.at[dz * 2 + dx], (zs[dz], y, 1 - xh if dx else xh, c, hd))

    for s in range(1, 4):
        for p in range(2):
            first_hop(s, p)
            second_hop(s - 1, p)
            if s > 1:
                last_hop(s - 2, p)
        if s == 2:
            send_queries()
    for p in range(2):
        second_hop(3, p)
        last_hop(2, p)
    for p in range(2):
        last_hop(3, p)

    for dz in range(4):
        for dx in range(2):
            if dz or dx:
                landed(q_out.at[zs[(4 - dz) % 4] * 2 + (1 - xh if dx else xh)], qr.at[dz * 2 + dx])
    for s in range(4):
        for i, yy in enumerate((y, down, up, over)):
            for p in range(2):
                landed(piece(came[s], yy, 1 - c, p), dd.at[s, i, p])
    for copy in sent:
        copy.wait_send()


def attend_kernel(kv, q, start_ref, o_ref, l_ref, plan, sm, low_s, bias_s, top_s, weight_s, acc_s, s_even, s_odd, sem):
    lane = lax.broadcasted_iota(jnp.int32, (1, 128), 1)
    lane32 = lax.broadcasted_iota(jnp.int32, (32, 128), 1)
    lane16 = lax.broadcasted_iota(jnp.int32, (16, 128), 1)
    code = lax.broadcasted_iota(jnp.int32, (32, 128), 0) * 2
    first = kv[:, 2 * GROUP, :].astype(jnp.float32).astype(jnp.int32)
    second = GROUPS - 1 - first
    at = jnp.where(first == lane32, code + 1, 0) + jnp.where(second == lane32, code + 2, 0)
    inv = jnp.sum(at, axis=0, keepdims=True) - 1
    here = jnp.where(inv >= 0, 1, 0)
    rank0 = jnp.sum(jnp.where(lane32 < first, here, 0), axis=1, keepdims=True)
    rank1 = jnp.sum(jnp.where(lane32 < second, here, 0), axis=1, keepdims=True)
    listed = jnp.where(rank0 == lane32, code * GROUPS, 0) + jnp.where(rank1 == lane32, (code + 1) * GROUPS, 0)
    plan[0:1, :] = jnp.sum(listed, axis=0, keepdims=True)
    plan[1:2, :] = inv

    q_first = q[:, 2 * GROUP, :].astype(jnp.float32).astype(jnp.int32)
    group = jnp.concatenate([q_first, GROUPS - 1 - q_first], axis=0)
    q_pos = group * GROUP + lane16
    low, low_first = jnp.zeros_like(q_pos), jnp.zeros_like(q_pos)
    for d in range(1, 16):
        begin = start_ref[d : d + 1, :]
        low = jnp.where(begin <= q_pos, begin, low)
        low_first = jnp.where(begin <= group * GROUP, begin, low_first)
    low_s[...] = low
    bias_s[...] = jnp.where(low == low_first, 0.0, MASKED)
    low_group = lax.shift_right_logical(low_first, 7)
    plan[16:32, :] = group
    plan[32:48, :] = low_group
    begin_at = jnp.sum(jnp.where(lane16 <= low_group, here, 0), axis=1, keepdims=True)
    end_at = jnp.sum(jnp.where(lane16 < group, here, 0), axis=1, keepdims=True)
    tiles = lax.shift_right_logical(jnp.maximum(end_at - begin_at, 0) + (TILE - 1), 2)
    begin_at, end_at, tiles = (jnp.broadcast_to(x, (16, 128)) for x in (begin_at, end_at, tiles))
    done = jnp.zeros((1, 128), jnp.int32)
    item = [lane, lane + 128, lane + 256]
    item_u, item_at, item_end = [[jnp.zeros((1, 128), jnp.int32) for _ in item] for _ in range(3)]
    for u in range(16):
        after = done + tiles[u : u + 1, :]
        for i, n in enumerate(item):
            mine = (done <= n) & (n < after)
            item_u[i] = jnp.where(mine, u, item_u[i])
            item_at[i] = jnp.where(mine, begin_at[u : u + 1, :] + (n - done) * TILE, item_at[i])
            item_end[i] = jnp.where(mine, end_at[u : u + 1, :], item_end[i])
        done = after
    for i in range(3):
        plan[2 + i : 3 + i, :] = item_u[i]
        plan[5 + i : 6 + i, :] = item_at[i]
        plan[8 + i : 9 + i, :] = item_end[i]
    plan[11:12, :] = done
    copy = pltpu.make_async_copy(plan, sm, sem)
    copy.start()
    copy.wait()

    row = lax.broadcasted_iota(jnp.int32, (GROUP, GROUP), 0)

    def half(slot, base):
        return pl.ds(pl.multiple_of(base + lax.rem(slot, 2) * GROUP, 16), GROUP)

    def queries_of(u):
        return q[lax.rem(u, 8), pl.ds(pl.multiple_of(lax.div(u, 8) * GROUP, GROUP), GROUP), :]

    def edges(u):
        g, low_g = sm[16 + u, 0], sm[32 + u, 0]
        q_t = queries_of(u)
        lower = low_s[pl.ds(u, 1), :]
        upper = g * GROUP + lane
        scores, held = [], []
        for key_group, wanted in ((g, True), (low_g, low_g < g)):
            found = sm[1, key_group]
            slot = jnp.maximum(found, 0)
            base = jnp.where((found >= 0) & wanted, key_group * GROUP, FAR)
            one = jnp.dot(kv[lax.div(slot, 2), half(slot, 0), :], q_t, preferred_element_type=jnp.float32)
            seen = (row >= lower - base) & (row <= upper - base)
            scores.append(jnp.where(seen, one, MASKED))
            held.append(kv[lax.div(slot, 2), half(slot, K_ROWS), :])
        top = jnp.full((1, GROUP), NEG, jnp.float32)
        for one in scores:
            top = jnp.maximum(top, jnp.max(one, axis=0, keepdims=True))
        parts = [jnp.exp2((one - top) * COEF) for one in scores]
        top_s[pl.ds(u, 1), :] = top
        weight_s[pl.ds(u, 1), :] = sum(jnp.sum(part, axis=0, keepdims=True) for part in parts)
        acc_s[u] = jnp.dot(
            jnp.concatenate(held, axis=1),
            jnp.concatenate([part.astype(jnp.bfloat16) for part in parts], axis=0),
            preferred_element_type=jnp.float32,
        )

    @pl.loop(0, 2)
    def _(k):
        for n in range(8):
            edges(8 * k + n)

    def read(i):
        r, k = lax.shift_right_logical(i, 7), lax.bitwise_and(i, 127)
        return sm[2 + r, k], sm[5 + r, k], sm[8 + r, k]

    def slot_of(e, end):
        return lax.shift_right_logical(sm[0, jnp.maximum(jnp.minimum(e, end - 1), 0)], 7)

    def score(i, dst):
        u, e, end = read(i)
        q_t = queries_of(u)
        for j in range(TILE):
            slot = slot_of(e + j, end)
            dst[j * GROUP : (j + 1) * GROUP, :] = jnp.dot(
                kv[lax.div(slot, 2), half(slot, 0), :], q_t, preferred_element_type=jnp.float32
            )

    def absorb(i, src):
        u, e, end = read(i)
        lanes = bias_s[pl.ds(u, 1), :]
        top = top_s[pl.ds(u, 1), :]
        new_top, biases, held, parts = top, [], [], []
        for j in range(TILE):
            biases.append(jnp.where(e + j < end, lanes, MASKED))
            best = jnp.max(src[j * GROUP : (j + 1) * GROUP, :], axis=0, keepdims=True)
            new_top = jnp.maximum(new_top, best + biases[j])
        factor = jnp.exp2((top - new_top) * COEF)
        weight = weight_s[pl.ds(u, 1), :] * factor
        for j in range(TILE):
            part = jnp.exp2((src[j * GROUP : (j + 1) * GROUP, :] - (new_top - biases[j])) * COEF)
            weight = weight + jnp.sum(part, axis=0, keepdims=True)
            parts.append(part.astype(jnp.bfloat16))
            slot = slot_of(e + j, end)
            held.append(kv[lax.div(slot, 2), half(slot, K_ROWS), :])
        top_s[pl.ds(u, 1), :] = new_top
        weight_s[pl.ds(u, 1), :] = weight
        acc_s[u] = acc_s[u] * factor + jnp.dot(
            jnp.concatenate(held, axis=1), jnp.concatenate(parts, axis=0), preferred_element_type=jnp.float32
        )

    total = sm[11, 0]
    score(jnp.int32(0), s_even)

    def run(first, count):
        for n in range(0, count, 2):
            i = first + n
            score(i + 1, s_odd)
            absorb(i, s_even)
            score(i + 2, s_even)
            absorb(i + 1, s_odd)

    sixteens = lax.shift_right_logical(total + 3, 4)

    @pl.loop(0, sixteens)
    def _(k):
        run(16 * k, 16)

    @pl.loop(0, lax.shift_right_logical(jnp.maximum(total - 16 * sixteens, 0) + 3, 2))
    def _(k):
        run(16 * sixteens + 4 * k, 4)

    @pl.loop(0, 16, unroll=4)
    def _(u):
        weight = weight_s[pl.ds(u, 1), :]
        some = weight > 0.0
        safe = jnp.where(some, weight, 1.0)
        ch, s = lax.rem(u, 8), lax.div(u, 8)
        o_ref[ch, pl.ds(pl.multiple_of(s * GROUP, GROUP), GROUP), :] = (acc_s[u] * (1.0 / safe)).astype(jnp.bfloat16)
        l_ref[ch, pl.ds(s, 1), :] = jnp.where(some, top_s[pl.ds(u, 1), :] * COEF + jnp.log2(safe), NEG)


def merge_kernel(o_ref, l_ref, out_ref, o_in, l_in, snd, orecv, lrecv):
    z, y, xh, c, hd = place()
    zs = [z, lax.rem(z + 1, 4), lax.rem(z + 2, 4), lax.rem(z + 3, 4)]
    peers = [(dz, dx) for dz in (2, 1, 3, 0) for dx in (1, 0) if dz or dx]
    barrier = pltpu.get_barrier_semaphore()
    for dz, dx in peers:
        to = (zs[dz], y, 1 - xh if dx else xh, c, hd)
        pl.semaphore_signal(barrier, inc=1, device_id=to, device_id_type=MESH)
    mine = z * 2 + xh
    pl.semaphore_wait(barrier, len(peers))
    sent = []
    for n, (dz, dx) in enumerate(peers):
        side = 1 - xh if dx else xh
        to, theirs = (zs[dz], y, side, c, hd), zs[dz] * 2 + side
        for src, dst, recv in ((o_ref, o_in, orecv), (l_ref, l_in, lrecv)):
            copy = remote(src.at[theirs], dst.at[mine], snd.at[len(sent)], recv.at[dz * 2 + dx], to)
            copy.start()
            sent.append(copy)
    o_in[mine] = o_ref[mine]
    l_in[mine] = l_ref[mine]
    for dz, dx in peers:
        side = 1 - xh if dx else xh
        theirs = zs[(4 - dz) % 4] * 2 + side
        to = (zs[1], y, xh, c, hd)
        remote(o_ref.at[0], o_in.at[theirs], snd.at[0], orecv.at[dz * 2 + dx], to).wait_recv()
        remote(l_ref.at[0], l_in.at[theirs], snd.at[0], lrecv.at[dz * 2 + dx], to).wait_recv()
    for h in range(4):
        for s in range(2):
            rows = slice(s * GROUP, (s + 1) * GROUP)
            a, b = l_in[2 * h, s : s + 1, :], l_in[2 * h + 1, s : s + 1, :]
            most = jnp.maximum(a, b)
            wa, wb = jnp.exp2(a - most), jnp.exp2(b - most)
            total = wa + wb
            merged = o_in[2 * h, rows, :].astype(jnp.float32) * (wa / total)
            merged = merged + o_in[2 * h + 1, rows, :].astype(jnp.float32) * (wb / total)
            out_ref[rows, h * HEAD_DIM : (h + 1) * HEAD_DIM] = merged.T.astype(jnp.bfloat16)
    for copy in sent:
        copy.wait_send()


def shards(queries, keys, values, group_table, doc_ids):
    vmem = pl.BlockSpec(memory_space=pltpu.VMEM)
    hbm = pl.BlockSpec(memory_space=pltpu.HBM)
    dma = pltpu.SemaphoreType.DMA
    kv, q, begins = pl.pallas_call(
        spread_kernel,
        out_shape=(
            pltpu.VMEM((32, CHUNK, HEAD_DIM), jnp.bfloat16),
            pltpu.VMEM((8, Q_ROWS, HEAD_DIM), jnp.bfloat16),
            pltpu.VMEM((16, 128), jnp.int32),
        ),
        in_specs=[hbm] * 5,
        out_specs=(vmem, vmem, vmem),
        scratch_shapes=[
            pltpu.VMEM((4, Q_AT + Q_ROWS, HEAD_DIM), jnp.bfloat16),
            pltpu.VMEM(queries.shape, jnp.bfloat16),
            pltpu.VMEM(values.shape, jnp.bfloat16),
            pltpu.VMEM((128, 128), jnp.int32),
            pltpu.SMEM((1, 2), jnp.int32),
            dma((8,)), dma((69,)), dma((4, 2)), dma((4, 2)), dma((4, 2)), dma((4, 2)), dma((4, 4, 2)), dma((8,)),
        ],
        compiler_params=pltpu.CompilerParams(collective_id=0, has_side_effects=True, vmem_limit_bytes=62050000),
    )(queries, keys, values, group_table, doc_ids.reshape(128, 128))
    o, l = pl.pallas_call(
        attend_kernel,
        out_shape=(
            pltpu.VMEM((8, 2 * GROUP, HEAD_DIM), jnp.bfloat16),
            pltpu.VMEM((8, 8, GROUP), jnp.float32),
        ),
        in_specs=[vmem, vmem, vmem],
        out_specs=(vmem, vmem),
        scratch_shapes=[
            pltpu.VMEM((48, 128), jnp.int32),
            pltpu.SMEM((48, 128), jnp.int32),
            pltpu.VMEM((16, 128), jnp.int32),
            pltpu.VMEM((16, 128), jnp.float32),
            pltpu.VMEM((16, 128), jnp.float32),
            pltpu.VMEM((16, 128), jnp.float32),
            pltpu.VMEM((16, HEAD_DIM, GROUP), jnp.float32),
            pltpu.VMEM((TILE * GROUP, GROUP), jnp.float32),
            pltpu.VMEM((TILE * GROUP, GROUP), jnp.float32),
            dma,
        ],
        compiler_params=pltpu.CompilerParams(vmem_limit_bytes=16 << 20),
    )(kv, q, begins)
    return pl.pallas_call(
        merge_kernel,
        out_shape=jax.ShapeDtypeStruct(queries.shape, jnp.bfloat16),
        in_specs=[vmem, vmem],
        out_specs=vmem,
        scratch_shapes=[
            pltpu.VMEM((8, 2 * GROUP, HEAD_DIM), jnp.bfloat16),
            pltpu.VMEM((8, 8, GROUP), jnp.float32),
            dma((14,)), dma((8,)), dma((8,)),
        ],
        compiler_params=pltpu.CompilerParams(collective_id=1, has_side_effects=True, vmem_limit_bytes=16 << 20),
    )(o, l)


def solution(mesh):
    split = Mesh(mesh.devices.reshape(4, 4, 2, 2, mesh.shape["head"]), AXES)
    return jax.shard_map(
        shards,
        mesh=split,
        in_specs=(P(BLK, "head"), P(BLK, "head"), P(BLK, "head"), P(BLK, None), P()),
        out_specs=P(BLK, "head"),
        check_vma=False,
    )
```

```python
import math

import jax
import jax.numpy as jnp
from jax import lax
from jax.experimental import pallas as pl
from jax.experimental.pallas import tpu as pltpu
from jax.sharding import Mesh
from jax.sharding import PartitionSpec as P

HEAD_DIM = 128
GROUP = 128
GROUPS = 128
AXES = ("z", "y", "xh", "core", "head")
BLK = AXES[:4]
MESH = pl.DeviceIdType.MESH
K_ROWS = 2 * GROUP + 16
CHUNK = K_ROWS + 2 * GROUP
Q_AT, Q_ROWS = CHUNK, 2 * GROUP + 16
NEG = -1e30
MASKED = -3e38
FAR = 1 << 20
TILE = 4
COEF = math.log2(math.e) / math.sqrt(HEAD_DIM)


def place():
    return tuple(lax.axis_index(a) for a in AXES)


def remote(src, dst, send, recv, to):
    return pltpu.make_async_remote_copy(
        src_ref=src, dst_ref=dst, send_sem=send, recv_sem=recv, device_id=to, device_id_type=MESH
    )


def spread_kernel(
    q_hbm, k_hbm, v_hbm, table_hbm, doc_hbm, kv_out, q_out, start_out, src, q_in, v_in, docs, table, loc, snd, own, yp, ym, rl, dd, qr
):
    z, y, xh, c, hd = place()
    up, down, over = lax.rem(y + 1, 4), lax.rem(y + 3, 4), lax.rem(y + 2, 4)
    zs = [z, lax.rem(z + 1, 4), lax.rem(z + 2, 4), lax.rem(z + 3, 4)]
    to_up, to_down, to_core = (z, up, xh, c, hd), (z, down, xh, c, hd), (z, y, xh, 1 - c, hd)
    local = [
        pltpu.make_async_copy(table_hbm, table, loc.at[0]),
        pltpu.make_async_copy(v_hbm, v_in, loc.at[1]),
        pltpu.make_async_copy(q_hbm, q_in, loc.at[2]),
        pltpu.make_async_copy(doc_hbm, docs, loc.at[3]),
    ]
    for h in range(4):
        keys_of_head = k_hbm.at[:, pl.ds(h * HEAD_DIM, HEAD_DIM)]
        local.append(pltpu.make_async_copy(keys_of_head, src.at[h, pl.ds(0, 2 * GROUP)], loc.at[4 + h]))
    for copy in local:
        copy.start()
    partners = [(zs[dz], y, xh, c, hd) for dz in (1, 2, 3)]
    partners += [(zs[dz], y, 1 - xh, c, hd) for dz in range(4)] + [to_up, to_down, to_core]
    barrier = pltpu.get_barrier_semaphore()
    for to in partners:
        pl.semaphore_signal(barrier, inc=1, device_id=to, device_id_type=MESH)

    local[0].wait()
    first = table[0, 0].astype(jnp.float32)
    for h in range(4):
        header = jnp.full((16, HEAD_DIM), first, jnp.float32).astype(jnp.bfloat16)
        src[h, K_ROWS - 16 : K_ROWS, :] = header
        src[h, Q_AT + 2 * GROUP :, :] = header
    local[1].wait()
    for h in range(4):
        for s in range(2):
            rows, cols = slice(s * GROUP, (s + 1) * GROUP), slice(h * HEAD_DIM, (h + 1) * HEAD_DIM)
            src[h, K_ROWS + s * GROUP : K_ROWS + (s + 1) * GROUP, :] = v_in[rows, cols].T
    for copy in local[2:]:
        copy.wait()
    pl.semaphore_wait(barrier, len(partners))

    sent = []

    def start(src_ref, dst_ref, recv, to):
        copy = remote(src_ref, dst_ref, snd.at[len(sent)], recv, to)
        copy.start()
        sent.append(copy)

    def landed(dst_ref, recv):
        remote(dst_ref, dst_ref, snd.at[0], recv, to_core).wait_recv()

    span = (pl.ds(0, K_ROWS), pl.ds(K_ROWS, 2 * GROUP))

    def piece(zz, yy, cc, p):
        return kv_out.at[(zz * 4 + yy) * 2 + cc, span[p]]

    order = (0, 1, 3, 2)
    came = [zs[(4 - dz) % 4] for dz in order]

    def first_hop(s, p):
        mine = piece(came[s], y, c, p)
        here = src.at[z, span[p]]
        if s > 0:
            landed(mine, own.at[s, p])
            here = mine
        start(here, mine, yp.at[s, p], to_up)
        start(here, mine, ym.at[s, p], to_down)
        start(here, mine, dd.at[s, 0, p], to_core)

    def second_hop(s, p):
        below, above = piece(came[s], down, c, p), piece(came[s], up, c, p)
        ways = [(below, yp, to_up, 1), (above, ym, to_down, 2)]
        for ref, came_in, onward, i in ways if p == 0 else ways[::-1]:
            landed(ref, came_in.at[s, p])
            if i == 1 + p:
                start(ref, ref, rl.at[s, p], onward)
            start(ref, ref, dd.at[s, i, p], to_core)

    def last_hop(s, p):
        across = piece(came[s], over, c, p)
        landed(across, rl.at[s, p])
        start(across, across, dd.at[s, 3, p], to_core)

    first_hop(0, 0)
    for s, p in ((1, 0), (2, 0), (1, 1), (2, 1), (3, 0), (3, 1)):
        dz = order[s]
        start(src.at[zs[dz], span[p]], piece(z, y, c, p), own.at[s, p], (zs[dz], y, xh, c, hd))
    first_hop(0, 1)
    kv_out[(z * 4 + y) * 2 + c] = src[z, 0:CHUNK]
    for h in range(4):
        for s in range(2):
            rows, cols = slice(s * GROUP, (s + 1) * GROUP), slice(h * HEAD_DIM, (h + 1) * HEAD_DIM)
            src[h, Q_AT + s * GROUP : Q_AT + (s + 1) * GROUP, :] = q_in[rows, cols].T
    held = docs[...]
    for d in range(16):
        counted = jnp.sum(jnp.where(held < d, 1, 0), axis=0, keepdims=True)
        start_out[d : d + 1, :] = jnp.broadcast_to(jnp.sum(counted, axis=1, keepdims=True), (1, 128))
    q_span, q_mine = pl.ds(Q_AT, Q_ROWS), q_out.at[z * 2 + xh]
    q_out[z * 2 + xh] = src[z, Q_AT:]
    def send_queries():
        for dz in (1, 3, 2, 0):
            for dx in (1, 0):
                if dz or dx:
                    start(src.at[zs[dz], q_span], q_mine, qr.at[dz * 2 + dx], (zs[dz], y, 1 - xh if dx else xh, c, hd))

    for s in range(1, 4):
        for p in range(2):
            first_hop(s, p)
            second_hop(s - 1, p)
            if s > 1:
                last_hop(s - 2, p)
        if s == 2:
            send_queries()
    for p in range(2):
        second_hop(3, p)
        last_hop(2, p)
    for p in range(2):
        last_hop(3, p)

    for dz in range(4):
        for dx in range(2):
            if dz or dx:
                landed(q_out.at[zs[(4 - dz) % 4] * 2 + (1 - xh if dx else xh)], qr.at[dz * 2 + dx])
    for s in range(4):
        for i, yy in enumerate((y, down, up, over)):
            for p in range(2):
                landed(piece(came[s], yy, 1 - c, p), dd.at[s, i, p])
    for copy in sent:
        copy.wait_send()


def attend_kernel(kv, q, start_ref, o_ref, l_ref, plan, sm, low_s, bias_s, top_s, weight_s, acc_s, s_even, s_odd, sem):
    lane = lax.broadcasted_iota(jnp.int32, (1, 128), 1)
    lane32 = lax.broadcasted_iota(jnp.int32, (32, 128), 1)
    lane16 = lax.broadcasted_iota(jnp.int32, (16, 128), 1)
    code = lax.broadcasted_iota(jnp.int32, (32, 128), 0) * 2
    first = kv[:, 2 * GROUP, :].astype(jnp.float32).astype(jnp.int32)
    second = GROUPS - 1 - first
    at = jnp.where(first == lane32, code + 1, 0) + jnp.where(second == lane32, code + 2, 0)
    inv = jnp.sum(at, axis=0, keepdims=True) - 1
    here = jnp.where(inv >= 0, 1, 0)
    rank0 = jnp.sum(jnp.where(lane32 < first, here, 0), axis=1, keepdims=True)
    rank1 = jnp.sum(jnp.where(lane32 < second, here, 0), axis=1, keepdims=True)
    listed = jnp.where(rank0 == lane32, code * GROUPS, 0) + jnp.where(rank1 == lane32, (code + 1) * GROUPS, 0)
    plan[0:1, :] = jnp.sum(listed, axis=0, keepdims=True)
    plan[1:2, :] = inv

    q_first = q[:, 2 * GROUP, :].astype(jnp.float32).astype(jnp.int32)
    group = jnp.concatenate([q_first, GROUPS - 1 - q_first], axis=0)
    q_pos = group * GROUP + lane16
    low, low_first = jnp.zeros_like(q_pos), jnp.zeros_like(q_pos)
    for d in range(1, 16):
        begin = start_ref[d : d + 1, :]
        low = jnp.where(begin <= q_pos, begin, low)
        low_first = jnp.where(begin <= group * GROUP, begin, low_first)
    low_s[...] = low
    bias_s[...] = jnp.where(low == low_first, 0.0, MASKED)
    low_group = lax.shift_right_logical(low_first, 7)
    plan[16:32, :] = group
    plan[32:48, :] = low_group
    begin_at = jnp.sum(jnp.where(lane16 <= low_group, here, 0), axis=1, keepdims=True)
    end_at = jnp.sum(jnp.where(lane16 < group, here, 0), axis=1, keepdims=True)
    tiles = lax.shift_right_logical(jnp.maximum(end_at - begin_at, 0) + (TILE - 1), 2)
    begin_at, end_at, tiles = (jnp.broadcast_to(x, (16, 128)) for x in (begin_at, end_at, tiles))
    done = jnp.zeros((1, 128), jnp.int32)
    item = [lane, lane + 128, lane + 256]
    item_u, item_at, item_end = [[jnp.zeros((1, 128), jnp.int32) for _ in item] for _ in range(3)]
    for u in range(16):
        after = done + tiles[u : u + 1, :]
        for i, n in enumerate(item):
            mine = (done <= n) & (n < after)
            item_u[i] = jnp.where(mine, u, item_u[i])
            item_at[i] = jnp.where(mine, begin_at[u : u + 1, :] + (n - done) * TILE, item_at[i])
            item_end[i] = jnp.where(mine, end_at[u : u + 1, :], item_end[i])
        done = after
    for i in range(3):
        plan[2 + i : 3 + i, :] = item_u[i]
        plan[5 + i : 6 + i, :] = item_at[i]
        plan[8 + i : 9 + i, :] = item_end[i]
    plan[11:12, :] = done
    copy = pltpu.make_async_copy(plan, sm, sem)
    copy.start()
    copy.wait()

    row = lax.broadcasted_iota(jnp.int32, (GROUP, GROUP), 0)

    def half(slot, base):
        return pl.ds(pl.multiple_of(base + lax.rem(slot, 2) * GROUP, 16), GROUP)

    def queries_of(u):
        return q[lax.rem(u, 8), pl.ds(pl.multiple_of(lax.div(u, 8) * GROUP, GROUP), GROUP), :]

    def edges(u):
        g, low_g = sm[16 + u, 0], sm[32 + u, 0]
        q_t = queries_of(u)
        lower = low_s[pl.ds(u, 1), :]
        upper = g * GROUP + lane
        scores, held = [], []
        for key_group, wanted in ((g, True), (low_g, low_g < g)):
            found = sm[1, key_group]
            slot = jnp.maximum(found, 0)
            base = jnp.where((found >= 0) & wanted, key_group * GROUP, FAR)
            one = jnp.dot(kv[lax.div(slot, 2), half(slot, 0), :], q_t, preferred_element_type=jnp.float32)
            seen = (row >= lower - base) & (row <= upper - base)
            scores.append(jnp.where(seen, one, MASKED))
            held.append(kv[lax.div(slot, 2), half(slot, K_ROWS), :])
        top = jnp.full((1, GROUP), NEG, jnp.float32)
        for one in scores:
            top = jnp.maximum(top, jnp.max(one, axis=0, keepdims=True))
        parts = [jnp.exp2((one - top) * COEF) for one in scores]
        top_s[pl.ds(u, 1), :] = top
        weight_s[pl.ds(u, 1), :] = sum(jnp.sum(part, axis=0, keepdims=True) for part in parts)
        acc_s[u] = jnp.dot(
            jnp.concatenate(held, axis=1),
            jnp.concatenate([part.astype(jnp.bfloat16) for part in parts], axis=0),
            preferred_element_type=jnp.float32,
        )

    @pl.loop(0, 1)
    def _(k):
        for n in range(16):
            edges(16 * k + n)

    def read(i):
        r, k = lax.shift_right_logical(i, 7), lax.bitwise_and(i, 127)
        return sm[2 + r, k], sm[5 + r, k], sm[8 + r, k]

    def slot_of(e, end):
        return lax.shift_right_logical(sm[0, jnp.maximum(jnp.minimum(e, end - 1), 0)], 7)

    def score(i, dst):
        u, e, end = read(i)
        q_t = queries_of(u)
        for j in range(TILE):
            slot = slot_of(e + j, end)
            dst[j * GROUP : (j + 1) * GROUP, :] = jnp.dot(
                kv[lax.div(slot, 2), half(slot, 0), :], q_t, preferred_element_type=jnp.float32
            )

    def absorb(i, src):
        u, e, end = read(i)
        lanes = bias_s[pl.ds(u, 1), :]
        top = top_s[pl.ds(u, 1), :]
        new_top, biases, held, parts = top, [], [], []
        for j in range(TILE):
            biases.append(jnp.where(e + j < end, lanes, MASKED))
            best = jnp.max(src[j * GROUP : (j + 1) * GROUP, :], axis=0, keepdims=True)
            new_top = jnp.maximum(new_top, best + biases[j])
        factor = jnp.exp2((top - new_top) * COEF)
        weight = weight_s[pl.ds(u, 1), :] * factor
        for j in range(TILE):
            part = jnp.exp2((src[j * GROUP : (j + 1) * GROUP, :] - (new_top - biases[j])) * COEF)
            weight = weight + jnp.sum(part, axis=0, keepdims=True)
            parts.append(part.astype(jnp.bfloat16))
            slot = slot_of(e + j, end)
            held.append(kv[lax.div(slot, 2), half(slot, K_ROWS), :])
        top_s[pl.ds(u, 1), :] = new_top
        weight_s[pl.ds(u, 1), :] = weight
        acc_s[u] = acc_s[u] * factor + jnp.dot(
            jnp.concatenate(held, axis=1), jnp.concatenate(parts, axis=0), preferred_element_type=jnp.float32
        )

    total = sm[11, 0]
    score(jnp.int32(0), s_even)

    def run(first, count):
        for n in range(0, count, 2):
            i = first + n
            score(i + 1, s_odd)
            absorb(i, s_even)
            score(i + 2, s_even)
            absorb(i + 1, s_odd)

    sixteens = lax.shift_right_logical(total + 3, 4)

    @pl.loop(0, sixteens)
    def _(k):
        run(16 * k, 16)

    @pl.loop(0, lax.shift_right_logical(jnp.maximum(total - 16 * sixteens, 0) + 3, 2))
    def _(k):
        run(16 * sixteens + 4 * k, 4)

    @pl.loop(0, 16, unroll=8)
    def _(u):
        weight = weight_s[pl.ds(u, 1), :]
        some = weight > 0.0
        safe = jnp.where(some, weight, 1.0)
        ch, s = lax.rem(u, 8), lax.div(u, 8)
        o_ref[ch, pl.ds(pl.multiple_of(s * GROUP, GROUP), GROUP), :] = (acc_s[u] * (1.0 / safe)).astype(jnp.bfloat16)
        l_ref[ch, pl.ds(s, 1), :] = jnp.where(some, top_s[pl.ds(u, 1), :] * COEF + jnp.log2(safe), NEG)


def merge_kernel(o_ref, l_ref, out_ref, o_in, l_in, snd, orecv, lrecv):
    z, y, xh, c, hd = place()
    zs = [z, lax.rem(z + 1, 4), lax.rem(z + 2, 4), lax.rem(z + 3, 4)]
    peers = [(dz, dx) for dz in (2, 1, 3, 0) for dx in (1, 0) if dz or dx]
    barrier = pltpu.get_barrier_semaphore()
    for dz, dx in peers:
        to = (zs[dz], y, 1 - xh if dx else xh, c, hd)
        pl.semaphore_signal(barrier, inc=1, device_id=to, device_id_type=MESH)
    mine = z * 2 + xh
    pl.semaphore_wait(barrier, len(peers))
    sent = []
    for n, (dz, dx) in enumerate(peers):
        side = 1 - xh if dx else xh
        to, theirs = (zs[dz], y, side, c, hd), zs[dz] * 2 + side
        for src, dst, recv in ((o_ref, o_in, orecv), (l_ref, l_in, lrecv)):
            copy = remote(src.at[theirs], dst.at[mine], snd.at[len(sent)], recv.at[dz * 2 + dx], to)
            copy.start()
            sent.append(copy)
    o_in[mine] = o_ref[mine]
    l_in[mine] = l_ref[mine]
    for dz, dx in peers:
        side = 1 - xh if dx else xh
        theirs = zs[(4 - dz) % 4] * 2 + side
        to = (zs[1], y, xh, c, hd)
        remote(o_ref.at[0], o_in.at[theirs], snd.at[0], orecv.at[dz * 2 + dx], to).wait_recv()
        remote(l_ref.at[0], l_in.at[theirs], snd.at[0], lrecv.at[dz * 2 + dx], to).wait_recv()
    for h in range(4):
        for s in range(2):
            rows = slice(s * GROUP, (s + 1) * GROUP)
            a, b = l_in[2 * h, s : s + 1, :], l_in[2 * h + 1, s : s + 1, :]
            most = jnp.maximum(a, b)
            wa, wb = jnp.exp2(a - most), jnp.exp2(b - most)
            total = wa + wb
            merged = o_in[2 * h, rows, :].astype(jnp.float32) * (wa / total)
            merged = merged + o_in[2 * h + 1, rows, :].astype(jnp.float32) * (wb / total)
            out_ref[rows, h * HEAD_DIM : (h + 1) * HEAD_DIM] = merged.T.astype(jnp.bfloat16)
    for copy in sent:
        copy.wait_send()


def shards(queries, keys, values, group_table, doc_ids):
    vmem = pl.BlockSpec(memory_space=pltpu.VMEM)
    hbm = pl.BlockSpec(memory_space=pltpu.HBM)
    dma = pltpu.SemaphoreType.DMA
    kv, q, begins = pl.pallas_call(
        spread_kernel,
        out_shape=(
            pltpu.VMEM((32, CHUNK, HEAD_DIM), jnp.bfloat16),
            pltpu.VMEM((8, Q_ROWS, HEAD_DIM), jnp.bfloat16),
            pltpu.VMEM((16, 128), jnp.int32),
        ),
        in_specs=[hbm] * 5,
        out_specs=(vmem, vmem, vmem),
        scratch_shapes=[
            pltpu.VMEM((4, Q_AT + Q_ROWS, HEAD_DIM), jnp.bfloat16),
            pltpu.VMEM(queries.shape, jnp.bfloat16),
            pltpu.VMEM(values.shape, jnp.bfloat16),
            pltpu.VMEM((128, 128), jnp.int32),
            pltpu.SMEM((1, 2), jnp.int32),
            dma((8,)), dma((69,)), dma((4, 2)), dma((4, 2)), dma((4, 2)), dma((4, 2)), dma((4, 4, 2)), dma((8,)),
        ],
        compiler_params=pltpu.CompilerParams(collective_id=0, has_side_effects=True, vmem_limit_bytes=62050000),
    )(queries, keys, values, group_table, doc_ids.reshape(128, 128))
    o, l = pl.pallas_call(
        attend_kernel,
        out_shape=(
            pltpu.VMEM((8, 2 * GROUP, HEAD_DIM), jnp.bfloat16),
            pltpu.VMEM((8, 8, GROUP), jnp.float32),
        ),
        in_specs=[vmem, vmem, vmem],
        out_specs=(vmem, vmem),
        scratch_shapes=[
            pltpu.VMEM((48, 128), jnp.int32),
            pltpu.SMEM((48, 128), jnp.int32),
            pltpu.VMEM((16, 128), jnp.int32),
            pltpu.VMEM((16, 128), jnp.float32),
            pltpu.VMEM((16, 128), jnp.float32),
            pltpu.VMEM((16, 128), jnp.float32),
            pltpu.VMEM((16, HEAD_DIM, GROUP), jnp.float32),
            pltpu.VMEM((TILE * GROUP, GROUP), jnp.float32),
            pltpu.VMEM((TILE * GROUP, GROUP), jnp.float32),
            dma,
        ],
        compiler_params=pltpu.CompilerParams(vmem_limit_bytes=16 << 20),
    )(kv, q, begins)
    return pl.pallas_call(
        merge_kernel,
        out_shape=jax.ShapeDtypeStruct(queries.shape, jnp.bfloat16),
        in_specs=[vmem, vmem],
        out_specs=vmem,
        scratch_shapes=[
            pltpu.VMEM((8, 2 * GROUP, HEAD_DIM), jnp.bfloat16),
            pltpu.VMEM((8, 8, GROUP), jnp.float32),
            dma((14,)), dma((8,)), dma((8,)),
        ],
        compiler_params=pltpu.CompilerParams(collective_id=1, has_side_effects=True, vmem_limit_bytes=16 << 20),
    )(o, l)


def solution(mesh):
    split = Mesh(mesh.devices.reshape(4, 4, 2, 2, mesh.shape["head"]), AXES)
    return jax.shard_map(
        shards,
        mesh=split,
        in_specs=(P(BLK, "head"), P(BLK, "head"), P(BLK, "head"), P(BLK, None), P()),
        out_specs=P(BLK, "head"),
        check_vma=False,
    )
```
